32 devices in a mesh: section: 2 (over core), dp: 4 (over z), mp: 4 (over y, x).
Axes of the slice: x: 2, y: 2, z: 4, core: 2. Of those that a mesh axis runs over, the one named last changes fastest.
Arguments:
- images: bfloat16 [12, 320, 1152], P('dp', 'mp'), may hold values from -6 to 6
- cotangent: bfloat16 [12, 320, 1152], P('dp', 'mp'), may hold values from -6 to 6
- lengths: int32 [12], P('dp'), may hold values from 192 to 320, as said below
- timesteps: int32 [12], P('dp'), may hold values from 0 to 999
- time_table: bfloat16 [1000, 1152], replicated, may hold values from -6 to 6
- norms: float32 [2, 4, 1152], P('section'), may hold values from 0.5 to 1.5
- qkv_weight: bfloat16 [2, 1152, 3, 1152], P('section', None, None, 'mp'), may hold values from -0.1875 to 0.1875
- time_weight: bfloat16 [2, 1152, 2, 1152], P('section', None, None, 'mp'), may hold values from -0.1875 to 0.1875
- out_weight: bfloat16 [2, 1152, 1152], P('section', 'mp'), may hold values from -0.75 to 0.75
- out_bias: float32 [2, 1152], P('section'), may hold values from -3 to 3
- mlp_in_weight: bfloat16 [2, 1152, 4608], P('section', None, 'mp'), may hold values from -0.1875 to 0.1875
- mlp_in_bias: float32 [2, 4608], P('section', 'mp'), may hold values from -3 to 3
- mlp_out_weight: bfloat16 [2, 4608, 1152], P('section', 'mp'), may hold values from -0.09375 to 0.09375
- mlp_out_bias: float32 [2, 1152], P('section'), may hold values from -3 to 3
- rel_bias: float32 [2, 16, 639], P('section', 'mp'), may hold values from -5 to 5
Outputs:
- boundary: float32 [2, 12, 320, 1152], P('section', 'dp', 'mp')
- grad_norms: float32 [2, 4, 1152], P('section')
- grad_qkv: float32 [2, 1152, 3, 1152], P('section', 'dp', None, 'mp')
- grad_time: float32 [2, 1152, 2, 1152], P('section', 'dp', None, 'mp')
- grad_out_weight: float32 [2, 1152, 1152], P('section', 'mp', 'dp')
- grad_out_bias: float32 [2, 1152], P('section')
- grad_mlp_in_weight: float32 [2, 1152, 4608], P('section', 'dp', 'mp')
- grad_mlp_in_bias: float32 [2, 4608], P('section', 'mp')
- grad_mlp_out_weight: float32 [2, 4608, 1152], P('section', 'mp', 'dp')
- grad_mlp_out_bias: float32 [2, 1152], P('section')
- grad_rel_bias: float32 [2, 16, 639], P('section', 'mp')
The draws below stay inside these ranges and needn't reach their ends.
Inputs may be any that keep to these rules, and one draw needn't show every extreme that they name: `lengths`: some image has exactly 320 tokens.
All inputs are finite; a program needn't handle non-finite values.
Results may differ from the reference program's by a relative error of at most 0.014.
The reference program's roundings to bfloat16 on the way count: a program that leaves them out, or rounds other values in their place, can miss the bound.
Values may be sent and summed in bfloat16 or wider, within the bound.
A program may use at most 192 MiB of HBM per device.

```python
import math
import jax
import jax.numpy as jnp
from jax import lax

D = 1152
H = 16
FF = 4608
LMAX = 320
NSTEPS = 1000
IMAGES = 12
OFFSETS = 639


def draw_lengths(key, part):
    first_key, second_key, third_key = jax.random.split(key, 3)
    shortest = LMAX * 3 // 5
    drawn = jax.random.randint(first_key, (IMAGES,), shortest, LMAX + 1)
    longest_at = jax.random.randint(second_key, (), 0, IMAGES)
    step_away = jax.random.randint(third_key, (), 1, IMAGES)
    shortest_at = (longest_at + step_away) % IMAGES
    places = jnp.arange(IMAGES)
    drawn = jnp.where(places == longest_at, LMAX, drawn)
    drawn = jnp.where(places == shortest_at, shortest, drawn)
    return drawn.astype(jnp.int32)


def plant(values, own_key, least, high):
    dims = values.shape
    index_at = [jax.random.randint(jax.random.fold_in(own_key, axis), (), 0, dims[axis]) for axis in range(len(dims))]
    values = values.at[tuple(index_at)].set(least)
    longest = dims.index(max(dims))
    index_at[longest] = (index_at[longest] + 1) % dims[longest]
    return values.at[tuple(index_at)].set(high)


def spiked(values, rng, source, target, blocks, factor):
    def block_of(axis_at):
        return (jnp.arange(values.shape[axis_at]) // (values.shape[axis_at] // blocks)).reshape((-1,) + (1,) * (values.ndim - 1 - axis_at))

    near = jax.random.permutation(rng, blocks)[block_of(target)]
    second = (block_of(target) + blocks // 2) % blocks
    return jnp.where((block_of(source) == near) | (block_of(source) == second), factor * values, values)


def block_scale(stream_key, extent, pieces, smallest, top_value):
    gain, own = 1.0, jax.random.fold_in(stream_key, 6)
    for dim, parts in pieces:
        heights = jnp.exp(jax.random.uniform(jax.random.fold_in(own, dim), (parts,), jnp.float32, smallest / len(pieces), top_value / len(pieces)))
        gain = gain * jnp.repeat(heights, extent[dim] // parts).reshape([-1 if axis == dim else 1 for axis in range(len(extent))])
    return gain


def scatter_about(stream_key, extent, deviation, limit, pieces=(), kind=jnp.bfloat16):
    values = deviation * jax.random.normal(stream_key, extent, jnp.float32)
    if pieces:
        values = values * block_scale(stream_key, extent, pieces, -0.22, 0.18)
    return jnp.clip(values, -limit, limit).astype(kind)


def bell_draw_with(own_key, shape, width, reach, cuts, heavy, kind=jnp.bfloat16):
    entries = width * jax.random.normal(own_key, shape, jnp.float32)
    if cuts:
        entries = entries * block_scale(own_key, shape, cuts, -0.22, 0.18)
    return jnp.clip(spiked(entries, jax.random.fold_in(own_key, 3), *heavy), -reach, reach).astype(kind)


def setup_inputs(seed: int = 0) -> dict:
    seeds = jax.random.split(jax.random.key(seed), 16)
    images = scatter_about(seeds[0], (IMAGES, LMAX, D), 1.0, 6.0, ((0, 4), (1, 4)))
    cotangent = bell_draw_with(seeds[1], (IMAGES, LMAX, D), 1.0, 6.0, ((0, 4), (1, 4)), (0, 2, 4, 2.0))
    lengths = draw_lengths(jax.random.fold_in(seeds[15], 71), 0)
    timesteps = plant(jax.random.randint(seeds[3], (IMAGES,), 0, NSTEPS), jax.random.fold_in(seeds[3], 1), 0, NSTEPS - 1).astype(jnp.int32)
    time_table = scatter_about(seeds[4], (NSTEPS, D), 1.0, 6.0)
    norms = jnp.clip(0.5 + 1.0 * jax.random.uniform(seeds[5], (2, 4, D), jnp.float32) ** block_scale(seeds[5], (2, 4, D), ((0, 2),), -0.2, 0.2), 0.5, 1.5)
    qkv_weight = scatter_about(seeds[6], (2, D, 3, D), D ** -0.5, 0.1875, ((0, 2), (3, 4)))
    time_weight = scatter_about(seeds[7], (2, D, 2, D), D ** -0.5, 0.1875, ((0, 2), (3, 4)))
    out_weight = scatter_about(seeds[8], (2, D, D), (D // 16) ** -0.5, 0.75, ((0, 2), (1, 4)))
    out_bias = scatter_about(seeds[9], (2, D), 0.5, 3.0, ((0, 2),), jnp.float32)
    mlp_in_weight = scatter_about(seeds[10], (2, D, FF), D ** -0.5, 0.1875, ((0, 2), (2, 4)))
    mlp_in_bias = scatter_about(seeds[11], (2, FF), 0.5, 3.0, ((0, 2), (1, 4)), jnp.float32)
    mlp_out_weight = scatter_about(seeds[12], (2, FF, D), FF ** -0.5, 0.09375, ((0, 2), (1, 4)))
    mlp_out_bias = scatter_about(seeds[13], (2, D), 0.5, 3.0, ((0, 2),), jnp.float32)
    rel_bias = scatter_about(seeds[14], (2, H, OFFSETS), 1.0, 5.0, ((0, 2), (1, 4)), jnp.float32)
    return dict(images=images, cotangent=cotangent, lengths=lengths, timesteps=timesteps, time_table=time_table, norms=norms, qkv_weight=qkv_weight, time_weight=time_weight, out_weight=out_weight, out_bias=out_bias, mlp_in_weight=mlp_in_weight, mlp_in_bias=mlp_in_bias, mlp_out_weight=mlp_out_weight, mlp_out_bias=mlp_out_bias, rel_bias=rel_bias)


@jax.custom_vjp
def low(v):
    return lax.optimization_barrier(v.astype(jnp.bfloat16)).astype(jnp.float32)

@jax.custom_vjp
def low_back(v):
    return v

def low_keep(v):
    return (low(v), None)

def low_pass(kept, grad):
    return (grad,)

def back_keep(v):
    return (v, None)

def back_low(kept, grad):
    return (low(grad),)
low.defvjp(low_keep, low_pass)
low_back.defvjp(back_keep, back_low)
EPSILON = 1e-06
NEG_FILL = -1000000000.0

def layer_norm(values, norm_gain, offset):
    centred = values - lax.optimization_barrier(jnp.mean(values, axis=-1, keepdims=True))
    spread = lax.optimization_barrier(jnp.mean(centred * centred, axis=-1, keepdims=True))
    return centred * lax.rsqrt(spread + EPSILON) * norm_gain + offset

def product(left, right):
    return jnp.dot(left, right, precision=lax.Precision.HIGHEST)

def image_block(params, image_item):
    tokens, length, time_token = image_item
    norm_rows, qkv_weight, time_weight, out_weight, out_bias, mlp_in_weight, mlp_in_bias, mlp_out_weight, mlp_out_bias, rel_bias = params
    seq_len = tokens.shape[0]
    model_width = tokens.shape[1]
    head_count = rel_bias.shape[0]
    head_size = model_width // head_count
    score_scale = 1.0 / math.sqrt(head_size)
    normed = low(layer_norm(tokens, norm_rows[0], norm_rows[1]))
    linear = product(normed, qkv_weight.reshape(model_width, 3 * model_width)).reshape(seq_len, 3, model_width)
    time_part = product(time_token[None, :], time_weight.reshape(model_width, 2 * model_width)).reshape(2, model_width)
    queries = low(low_back(linear[:, 0] + time_part[0])).reshape(seq_len, head_count, head_size)
    key_rows = low(low_back(linear[:, 1])).reshape(seq_len, head_count, head_size)
    values = low(low_back(linear[:, 2] + time_part[1])).reshape(seq_len, head_count, head_size)
    positions = jnp.arange(seq_len, dtype=jnp.int32)
    offsets = positions[:, None] - positions[None, :] + (seq_len - 1)
    scores = jnp.einsum('qhd,khd->hqk', queries, key_rows, precision=lax.Precision.HIGHEST) * score_scale + rel_bias[:, offsets]
    scores = low_back(scores)
    scores = jnp.where((positions < length)[None, None, :], scores, NEG_FILL)
    probability = jax.nn.softmax(scores, axis=-1)
    attended = jnp.einsum('hqk,khd->qhd', low(probability), values, precision=lax.Precision.HIGHEST)
    attended = low(low_back(attended)).reshape(seq_len, model_width)
    mixed_rows = tokens + low_back(product(attended, out_weight) + out_bias)
    normed_two = low(layer_norm(mixed_rows, norm_rows[2], norm_rows[3]))
    hidden = low_back(product(normed_two, mlp_in_weight) + mlp_in_bias)
    activated = low(jax.nn.gelu(hidden))
    return mixed_rows + low_back(product(activated, mlp_out_weight) + mlp_out_bias)

def run_layer(params, tokens, lengths, time_tokens):
    checked_block = jax.checkpoint(image_block)
    return lax.map(lambda image_item: checked_block(params, image_item), (tokens, lengths, time_tokens))

def reference(images, cotangent, lengths, timesteps, time_table, norms, qkv_weight, time_weight, out_weight, out_bias, mlp_in_weight, mlp_in_bias, mlp_out_weight, mlp_out_bias, rel_bias):
    layer_params = (norms, qkv_weight.astype(jnp.float32), time_weight.astype(jnp.float32), out_weight.astype(jnp.float32), out_bias, mlp_in_weight.astype(jnp.float32), mlp_in_bias, mlp_out_weight.astype(jnp.float32), mlp_out_bias, rel_bias)
    time_tokens = time_table.astype(jnp.float32)[timesteps]
    seq_len = images.shape[1]
    row_mask = (jnp.arange(seq_len, dtype=jnp.int32)[None, :] < lengths[:, None]).astype(jnp.float32)[:, :, None]

    def forward(inputs, params):
        first_layer = jax.tree.map(lambda array_leaf: array_leaf[0], params)
        second_layer = jax.tree.map(lambda array_leaf: array_leaf[1], params)
        middle = run_layer(first_layer, inputs, lengths, time_tokens)
        middle = low(low_back(middle))
        return run_layer(second_layer, middle, lengths, time_tokens)
    outputs, pullback = jax.vjp(forward, images.astype(jnp.float32), layer_params)
    grad_inputs, gradients = pullback(cotangent.astype(jnp.float32) * row_mask)
    boundary = jnp.stack([grad_inputs, outputs * row_mask])
    return (boundary, gradients[0], gradients[1], gradients[2], gradients[3], gradients[4], gradients[5], gradients[6], gradients[7], gradients[8], gradients[9])
```

```python
import math

import jax
import jax.numpy as jnp
from jax import lax
from jax.sharding import PartitionSpec as P

EPSILON = 1e-06
NEG_FILL = -1000000000.0


def from_behind(array, axis, by):
    size = lax.axis_size(axis)
    pairs = [(i, i + by) for i in range(size) if 0 <= i + by < size]
    return lax.ppermute(array, axis, pairs)


def layer_norm(values, norm_gain, offset):
    centred = values - jnp.mean(values, axis=-1, keepdims=True)
    spread = jnp.mean(centred * centred, axis=-1, keepdims=True)
    return centred * lax.rsqrt(spread + EPSILON) * norm_gain + offset


def toeplitz(table):
    head_count, offset_count = table.shape
    seq_len = (offset_count + 1) // 2
    flipped = jnp.flip(table, axis=1)
    extended = jnp.concatenate([flipped, jnp.zeros((head_count, 1), jnp.float32)], axis=1)
    repeated = jnp.broadcast_to(extended[:, None, :], (head_count, seq_len, 2 * seq_len))
    repeated = repeated.reshape(head_count, 2 * seq_len * seq_len)
    skewed = repeated[:, seq_len - 1 : seq_len - 1 + seq_len * offset_count]
    return skewed.reshape(head_count, seq_len, offset_count)[:, :, :seq_len]


def widen_rows(rows_low):
    return lax.all_gather(rows_low, "mp", axis=0, tiled=True)


def narrow_rows(left, weight):
    return lax.psum_scatter(
        jnp.dot(left, weight, preferred_element_type=jnp.float32).astype(jnp.bfloat16),
        "mp",
        scatter_dimension=0,
        tiled=True,
    ).astype(jnp.float32)


def grad_widen_rows(rows_low):
    return lax.all_gather(rows_low, "mp", axis=0, tiled=True)


def grad_narrow_rows(left, weight):
    return lax.psum_scatter(
        lax.dot_general(
            left, weight, (((1,), (1,)), ((), ())), preferred_element_type=jnp.float32
        ).astype(jnp.bfloat16),
        "mp",
        scatter_dimension=0,
        tiled=True,
    ).astype(jnp.float32)


def attention_scores(queries, key_rows, bias_full, key_mask):
    score_scale = 1.0 / math.sqrt(queries.shape[2])
    raw_scores = (
        jnp.einsum("qhd,khd->hqk", queries, key_rows, preferred_element_type=jnp.float32)
        * score_scale
        + bias_full
    )
    return jnp.where(key_mask[None, None, :], raw_scores, NEG_FILL)


def layer_forward(tokens, length, time_token, layer_params):
    (
        norm_rows,
        qkv_flat,
        time_flat,
        out_weight,
        out_bias,
        mlp_in_weight,
        mlp_in_bias,
        mlp_out_weight,
        mlp_out_bias,
        bias_full,
    ) = layer_params
    normed, norm_pull = jax.vjp(layer_norm, tokens, norm_rows[0], norm_rows[1])
    normed_full = widen_rows(normed.astype(jnp.bfloat16))
    seq_len = normed_full.shape[0]
    local_width = qkv_flat.shape[1] // 3
    head_count = bias_full.shape[0]
    head_size = local_width // head_count
    linear = jnp.dot(normed_full, qkv_flat, preferred_element_type=jnp.float32)
    time_part = jnp.dot(time_token[None, :], time_flat, preferred_element_type=jnp.float32)
    queries = (linear[:, :local_width] + time_part[:, :local_width]).astype(jnp.bfloat16)
    key_rows = linear[:, local_width : 2 * local_width].astype(jnp.bfloat16)
    values = (linear[:, 2 * local_width :] + time_part[:, local_width:]).astype(jnp.bfloat16)
    queries = queries.reshape(seq_len, head_count, head_size)
    key_rows = key_rows.reshape(seq_len, head_count, head_size)
    values = values.reshape(seq_len, head_count, head_size)
    key_mask = jnp.arange(seq_len, dtype=jnp.int32) < length
    scores = attention_scores(queries, key_rows, bias_full, key_mask)
    row_peak = jnp.max(scores, axis=-1, keepdims=True)
    log_total = row_peak + jnp.log(jnp.sum(jnp.exp(scores - row_peak), axis=-1, keepdims=True))
    probability = jnp.exp(scores - log_total)
    attended = jnp.einsum(
        "hqk,khd->qhd", probability.astype(jnp.bfloat16), values, preferred_element_type=jnp.float32
    )
    attended = attended.reshape(seq_len, local_width).astype(jnp.bfloat16)
    mixed_rows = tokens + narrow_rows(attended, out_weight) + out_bias
    normed_two, norm_pull_two = jax.vjp(layer_norm, mixed_rows, norm_rows[2], norm_rows[3])
    normed_two_full = widen_rows(normed_two.astype(jnp.bfloat16))
    hidden = (
        jnp.dot(normed_two_full, mlp_in_weight, preferred_element_type=jnp.float32) + mlp_in_bias
    )
    activated = jax.nn.gelu(hidden).astype(jnp.bfloat16)
    output = mixed_rows + narrow_rows(activated, mlp_out_weight) + mlp_out_bias
    kept = (
        norm_pull,
        normed_full,
        queries,
        key_rows,
        values,
        probability,
        attended,
        norm_pull_two,
        normed_two_full,
        hidden,
        activated,
    )
    return (output, kept)


def layer_backward(kept, layer_params, grad_out):
    (
        norm_rows,
        qkv_flat,
        time_flat,
        out_weight,
        out_bias,
        mlp_in_weight,
        mlp_in_bias,
        mlp_out_weight,
        mlp_out_bias,
        bias_full,
    ) = layer_params
    (
        norm_pull,
        normed_full,
        queries,
        key_rows,
        values,
        probability,
        attended,
        norm_pull_two,
        normed_two_full,
        hidden,
        activated,
    ) = kept
    seq_len = normed_full.shape[0]
    local_width = qkv_flat.shape[1] // 3
    head_count = bias_full.shape[0]
    head_size = local_width // head_count
    score_scale = 1.0 / math.sqrt(head_size)
    contract_rows = (((0,), (0,)), ((), ()))
    contract_cols = (((1,), (1,)), ((), ()))
    grad_branch_two = grad_out.astype(jnp.bfloat16)
    mlp_out_bias_grad = jnp.sum(grad_branch_two.astype(jnp.float32), axis=0)
    grad_two_full = grad_widen_rows(grad_branch_two)
    mlp_out_grad = lax.dot_general(
        activated, grad_two_full, contract_rows, preferred_element_type=jnp.float32
    )
    grad_activated = lax.dot_general(
        grad_two_full, mlp_out_weight, contract_cols, preferred_element_type=jnp.float32
    )
    _, gelu_pull = jax.vjp(jax.nn.gelu, hidden)
    grad_hidden = gelu_pull(grad_activated)[0].astype(jnp.bfloat16)
    mlp_in_bias_grad = jnp.sum(grad_hidden.astype(jnp.float32), axis=0)
    mlp_in_grad = lax.dot_general(
        normed_two_full, grad_hidden, contract_rows, preferred_element_type=jnp.float32
    )
    grad_normed_two = grad_narrow_rows(grad_hidden, mlp_in_weight)
    grad_mixed_part, gain_two_grad, offset_two_grad = norm_pull_two(grad_normed_two)
    grad_mixed = grad_out + grad_mixed_part
    grad_branch = grad_mixed.astype(jnp.bfloat16)
    out_bias_grad = jnp.sum(grad_branch.astype(jnp.float32), axis=0)
    grad_branch_full = grad_widen_rows(grad_branch)
    out_grad = lax.dot_general(
        attended, grad_branch_full, contract_rows, preferred_element_type=jnp.float32
    )
    grad_attended = lax.dot_general(
        grad_branch_full, out_weight, contract_cols, preferred_element_type=jnp.float32
    )
    grad_attended = grad_attended.astype(jnp.bfloat16).reshape(seq_len, head_count, head_size)
    grad_probability = jnp.einsum(
        "qhd,khd->hqk", grad_attended, values, preferred_element_type=jnp.float32
    )
    grad_values = jnp.einsum(
        "hqk,qhd->khd",
        probability.astype(jnp.bfloat16),
        grad_attended,
        preferred_element_type=jnp.float32,
    )
    row_inner = jnp.sum(probability * grad_probability, axis=-1, keepdims=True)
    grad_scores = (probability * (grad_probability - row_inner)).astype(jnp.bfloat16)
    grad_queries = (
        jnp.einsum("hqk,khd->qhd", grad_scores, key_rows, preferred_element_type=jnp.float32)
        * score_scale
    )
    grad_keys = (
        jnp.einsum("hqk,qhd->khd", grad_scores, queries, preferred_element_type=jnp.float32)
        * score_scale
    )
    grad_project = jnp.concatenate(
        [
            grad_queries.reshape(seq_len, local_width),
            grad_keys.reshape(seq_len, local_width),
            grad_values.reshape(seq_len, local_width),
        ],
        axis=1,
    ).astype(jnp.bfloat16)
    qkv_grad = lax.dot_general(
        normed_full, grad_project, contract_rows, preferred_element_type=jnp.float32
    )
    column_sums = jnp.sum(grad_project.astype(jnp.float32), axis=0)
    time_columns = jnp.concatenate([column_sums[:local_width], column_sums[2 * local_width :]])
    grad_normed = grad_narrow_rows(grad_project, qkv_flat)
    grad_tokens_part, gain_grad, offset_grad = norm_pull(grad_normed)
    grad_tokens = grad_mixed + grad_tokens_part
    norms_grad = jnp.stack([gain_grad, offset_grad, gain_two_grad, offset_two_grad])
    gradients = (
        norms_grad,
        qkv_grad,
        time_columns,
        out_grad,
        out_bias_grad,
        mlp_in_grad,
        mlp_in_bias_grad,
        mlp_out_grad,
        mlp_out_bias_grad,
        grad_scores.astype(jnp.float32),
    )
    return (grad_tokens, gradients)


def write_slot(store, slot_index, value, active):
    previous = lax.dynamic_index_in_dim(store, slot_index, 0, keepdims=False)
    return lax.dynamic_update_index_in_dim(store, jnp.where(active, value, previous), slot_index, 0)


def local(
    images,
    cotangent,
    lengths,
    timesteps,
    time_table,
    norms,
    qkv_weight,
    time_weight,
    out_weight,
    out_bias,
    mlp_in_weight,
    mlp_in_bias,
    mlp_out_weight,
    mlp_out_bias,
    rel_bias,
):
    model_rank = lax.axis_index("mp")
    section_rank = lax.axis_index("section")
    micro_total = images.shape[0]
    row_count = images.shape[1]
    model_width = images.shape[2]
    local_width = qkv_weight.shape[3]
    qkv_flat = qkv_weight[0].reshape(model_width, 3 * local_width)
    time_flat = time_weight[0].reshape(model_width, 2 * local_width)
    bias_full, bias_pull = jax.vjp(toeplitz, rel_bias[0])
    layer_params = (
        norms[0],
        qkv_flat,
        time_flat,
        out_weight[0],
        out_bias[0],
        mlp_in_weight[0],
        mlp_in_bias[0],
        mlp_out_weight[0],
        mlp_out_bias[0],
        bias_full,
    )
    row_index = model_rank * row_count + jnp.arange(row_count, dtype=jnp.int32)

    def image_inputs(slot_index):
        length = lax.dynamic_index_in_dim(lengths, slot_index, 0, keepdims=False)
        step_index = lax.dynamic_index_in_dim(timesteps, slot_index, 0, keepdims=False)
        time_token = lax.dynamic_index_in_dim(time_table, step_index, 0, keepdims=False)
        row_mask = (row_index < length).astype(jnp.float32)[:, None]
        return (length, time_token, row_mask)

    kept_ticks = []
    boundary = jnp.zeros((micro_total, row_count, model_width), jnp.float32)
    received = jnp.zeros((row_count, model_width), jnp.bfloat16)
    for tick_index in range(micro_total + 1):
        micro_index = tick_index - section_rank
        active = (micro_index >= 0) & (micro_index < micro_total)
        slot_index = jnp.clip(micro_index, 0, micro_total - 1)
        length, time_token, row_mask = image_inputs(slot_index)
        arriving = jnp.where(section_rank == 0, images[min(tick_index, micro_total - 1)], received)
        output, kept = layer_forward(
            arriving.astype(jnp.float32), length, time_token, layer_params
        )
        kept_ticks.append(kept)
        boundary = write_slot(boundary, slot_index, output * row_mask, active & (section_rank == 1))
        if tick_index < micro_total:
            received = from_behind(output.astype(jnp.bfloat16), "section", 1)
    totals = None
    time_slots = jnp.zeros((micro_total, 2 * local_width), jnp.float32)
    incoming = jnp.zeros((row_count, model_width), jnp.bfloat16)
    for tick_index in range(micro_total + 1):
        micro_index = micro_total - tick_index - section_rank
        active = (micro_index >= 0) & (micro_index < micro_total)
        slot_index = jnp.clip(micro_index, 0, micro_total - 1)
        length, time_token, row_mask = image_inputs(slot_index)
        given_grad = cotangent[max(micro_total - 1 - tick_index, 0)].astype(jnp.float32) * row_mask
        grad_out = jnp.where(section_rank == 1, given_grad, incoming.astype(jnp.float32))
        grad_out = jnp.where(active, grad_out, 0.0)
        grad_tokens, gradients = layer_backward(
            kept_ticks[micro_total - tick_index], layer_params, grad_out
        )
        columns = gradients[2]
        gradients = gradients[:2] + (jnp.zeros((), jnp.float32),) + gradients[3:]
        time_slots = write_slot(time_slots, slot_index, columns, active)
        if totals is None:
            totals = gradients
        else:
            totals = jax.tree.map(jnp.add, totals, gradients)
        boundary = write_slot(boundary, slot_index, grad_tokens, active & (section_rank == 0))
        if tick_index < micro_total:
            incoming = from_behind(grad_tokens.astype(jnp.bfloat16), "section", -1)
    final_qkv = totals[1].reshape(model_width, 3, local_width)
    final_out, final_mlp_in, final_mlp_out = totals[3], totals[5], totals[7]
    all_slots = lax.all_gather(time_slots, "dp", axis=0, tiled=True)
    all_steps = lax.all_gather(timesteps, "dp", axis=0, tiled=True)
    share = model_width // lax.axis_size("dp")
    time_rows = lax.dynamic_slice_in_dim(
        time_table[all_steps], lax.axis_index("dp") * share, share, axis=1
    )
    time_grad = lax.dot_general(
        time_rows.astype(jnp.float32),
        all_slots,
        (((0,), (0,)), ((), ())),
        precision=lax.Precision.HIGHEST,
        preferred_element_type=jnp.float32,
    ).reshape(share, 2, local_width)
    summed = (
        lax.psum_scatter(
            final_qkv.astype(jnp.bfloat16), "dp", scatter_dimension=0, tiled=True
        ).astype(jnp.float32),
        time_grad,
        lax.psum_scatter(
            final_out.astype(jnp.bfloat16), "dp", scatter_dimension=1, tiled=True
        ).astype(jnp.float32),
        lax.psum_scatter(
            final_mlp_in.astype(jnp.bfloat16), "dp", scatter_dimension=0, tiled=True
        ).astype(jnp.float32),
        lax.psum_scatter(
            final_mlp_out.astype(jnp.bfloat16), "dp", scatter_dimension=1, tiled=True
        ).astype(jnp.float32),
    )
    rel_grad = bias_pull(totals[9])[0]
    table_sum = lax.psum((rel_grad, totals[6]), "dp")
    shared = lax.psum((totals[0], totals[4], totals[8]), ("dp", "mp"))
    return (
        boundary[None],
        shared[0][None],
        summed[0][None],
        summed[1][None],
        summed[2][None],
        shared[1][None],
        summed[3][None],
        table_sum[1][None],
        summed[4][None],
        shared[2][None],
        table_sum[0][None],
    )


def solution(mesh):
    in_specs = (
        P("dp", "mp", None),
        P("dp", "mp", None),
        P("dp"),
        P("dp"),
        P(),
        P("section", None, None),
        P("section", None, None, "mp"),
        P("section", None, None, "mp"),
        P("section", "mp", None),
        P("section", None),
        P("section", None, "mp"),
        P("section", "mp"),
        P("section", "mp", None),
        P("section", None),
        P("section", "mp", None),
    )
    out_specs = (
        P("section", "dp", "mp", None),
        P("section", None, None),
        P("section", "dp", None, "mp"),
        P("section", "dp", None, "mp"),
        P("section", "mp", "dp"),
        P("section", None),
        P("section", "dp", "mp"),
        P("section", "mp"),
        P("section", "mp", "dp"),
        P("section", None),
        P("section", "mp", None),
    )
    return jax.shard_map(local, mesh=mesh, in_specs=in_specs, out_specs=out_specs, check_vma=False)
```

```python
import functools
import math

import jax
import jax.numpy as jnp
from jax import lax
from jax.experimental import pallas as pl
from jax.experimental.pallas import tpu as pltpu
from jax.sharding import PartitionSpec as P

EPSILON = 1e-06
NEG_FILL = -1000000000.0
LANES = 128
BF = jnp.bfloat16
F32 = jnp.float32
ROOT = math.sqrt(2.0 / math.pi)
CUBIC = 0.044715


def mm(left, right, left_dim=1, right_dim=0):
    return lax.dot_general(
        left, right, (((left_dim,), (right_dim,)), ((), ())), preferred_element_type=F32
    )


def selection(rows, cols, head_size, flip):
    shape = (cols, rows) if flip else (rows, cols)
    row = lax.broadcasted_iota(jnp.int32, shape, 1 if flip else 0)
    col = lax.broadcasted_iota(jnp.int32, shape, 0 if flip else 1)
    within = col & (LANES - 1)
    hit = (within < head_size) & (row == (col // LANES) * head_size + within)
    return jnp.where(hit, 1.0, 0.0).astype(BF)


def normalize(values):
    centred = values - jnp.mean(values, axis=-1, keepdims=True)
    spread = jnp.mean(centred * centred, axis=-1, keepdims=True)
    scale = lax.rsqrt(spread + EPSILON)
    return centred * scale, scale


def norm_backward(grad, values, gain):
    unit, scale = normalize(values)
    inner = grad * gain
    mean_one = jnp.mean(inner, axis=-1, keepdims=True)
    mean_two = jnp.mean(inner * unit, axis=-1, keepdims=True)
    grad_in = scale * (inner - mean_one - unit * mean_two)
    gain_grad = jnp.sum(grad * unit, axis=0, keepdims=True)
    offset_grad = jnp.sum(grad, axis=0, keepdims=True)
    return grad_in, gain_grad, offset_grad


def layer_kernel(
    sizes,
    lengths_ref,
    images_ref,
    cotangent_ref,
    time_ref,
    norms_ref,
    qkv_raw_ref,
    out_w_ref,
    out_b_ref,
    in_w_ref,
    in_b_ref,
    back_w_ref,
    back_b_ref,
    table_ref,
    boundary_ref,
    small_ref,
    table_grad_ref,
    columns_ref,
    qkv_grad_ref,
    out_grad_ref,
    in_grad_ref,
    back_grad_ref,
    w_raw,
    w_qkv,
    w_out,
    w_in,
    w_back,
    normed,
    normed_two,
    grad_two,
    grad_one,
    active,
    grad_hidden,
    qkv,
    mixed_heads,
    grad_qkv,
    probs,
    slope,
    bias,
    score_sum,
    parts,
    sends,
    tokens,
    passed,
    mixed,
    stage,
    thin_stage,
    load_sem,
    gather_send,
    gather_recv,
    part_send,
    part_recv,
    pass_send,
    pass_recv,
    store_sem,
):
    n, count, rows, width, hidden_width, heads, head_size, shares = sizes
    seq = n * rows
    local = heads * head_size
    wide = heads * LANES
    share = width // shares
    score_scale = 1.0 / math.sqrt(head_size)
    me = lax.axis_index("mp")
    section = lax.axis_index("section")
    own = pl.multiple_of(me * rows, 16)

    def peer(d):
        return lax.rem(me + d, n)

    def source(d):
        return lax.rem(me + n - d, n)

    barrier = pltpu.get_barrier_semaphore()
    for d in range(1, n):
        pl.semaphore_signal(barrier, inc=1, device_id={"mp": peer(d)})
    pl.semaphore_signal(barrier, inc=1, device_id={"section": 1 - section})
    pl.semaphore_wait(barrier, n)

    loads = [
        pltpu.make_async_copy(a, b, load_sem.at[k])
        for k, (a, b) in enumerate(
            [(qkv_raw_ref, w_raw), (out_w_ref, w_out), (in_w_ref, w_in), (back_w_ref, w_back)]
        )
    ]
    for load in loads:
        load.start()

    def rows_of(i, index):
        return pl.ds(pl.multiple_of(i * seq + index * rows, 16), rows)

    def image_of(i):
        return pl.ds(pl.multiple_of(i * seq, 16), seq)

    def gather_copy(kind, buf, i, d, index):
        where = rows_of(i, index)
        return pltpu.make_async_remote_copy(
            src_ref=buf.at[where],
            dst_ref=buf.at[where],
            send_sem=gather_send.at[kind, i, d - 1],
            recv_sem=gather_recv.at[kind, i, d - 1],
            device_id={"mp": peer(d)},
        )

    def gather_start(kind, buf, i):
        for d in range(1, n):
            gather_copy(kind, buf, i, d, me).start()

    def gather_wait(kind, buf, i):
        for d in range(1, n):
            gather_copy(kind, buf, i, d, me).wait_send()
            gather_copy(kind, buf, i, d, source(d)).wait_recv()

    def part_copy(kind, i, d):
        return pltpu.make_async_remote_copy(
            src_ref=sends.at[rows_of(i, peer(d))],
            dst_ref=parts.at[kind & 1, i, d - 1],
            send_sem=part_send.at[kind, i, d - 1],
            recv_sem=part_recv.at[kind, i, d - 1],
            device_id={"mp": peer(d)},
        )

    def part_start(kind, i):
        for d in range(1, n):
            part_copy(kind, i, d).start()

    def part_sum(kind, i):
        for d in range(1, n):
            part_copy(kind, i, d).wait()
        total = sends[rows_of(i, me), :].astype(F32)
        for d in range(1, n):
            total = total + parts[kind & 1, i, d - 1].astype(F32)
        return total

    def pass_copy(k, i, dst):
        return pltpu.make_async_remote_copy(
            src_ref=passed.at[i],
            dst_ref=dst,
            send_sem=pass_send.at[k, i],
            recv_sem=pass_recv.at[k, i],
            device_id={"section": 1 - section},
        )

    def row_mask(i):
        index = me * rows + lax.broadcasted_iota(jnp.int32, (rows, 1), 0)
        return index < lengths_ref[i]

    def enter(i):
        @pl.when(section == 1)
        def _():
            pass_copy(0, i, tokens.at[i]).wait_recv()

        unit, _ = normalize(tokens[i].astype(F32))
        normed[rows_of(i, me), :] = (unit * norms_ref[0:1, :] + norms_ref[1:2, :]).astype(BF)
        gather_start(0, normed, i)

    def attend(i):
        gather_wait(0, normed, i)
        here = image_of(i)
        for j in range(3):
            linear = mm(normed[here, :], w_qkv[j])
            if j == 0:
                linear = linear + time_ref[i, 0:1, :]
            if j == 2:
                linear = linear + time_ref[i, 1:2, :]
            qkv[j, here, :] = linear.astype(BF)
        key_index = lax.broadcasted_iota(jnp.int32, (1, seq), 1)
        key_mask = key_index < lengths_ref[i]
        outs = []
        for h in range(heads):
            lanes = slice(h * LANES, (h + 1) * LANES)
            scores = mm(qkv[0, here, lanes], qkv[1, here, lanes], 1, 1) * score_scale + bias[h]
            scores = jnp.where(key_mask, scores, NEG_FILL)
            top = jnp.max(scores, axis=-1, keepdims=True)
            raised = jnp.exp(scores - top)
            prob = raised / jnp.sum(raised, axis=-1, keepdims=True)
            probs[i * heads + h] = prob
            outs.append(mm(prob.astype(BF), qkv[2, here, lanes]).astype(BF))
        packed = mm(jnp.concatenate(outs, axis=1), selection(local, wide, head_size, True))
        packed = packed.astype(BF)
        mixed_heads[here, :] = packed
        sends[here, :] = mm(packed, w_out[...]).astype(BF)
        part_start(0, i)

    def middle(i):
        total = tokens[i].astype(F32) + part_sum(0, i) + out_b_ref[...]
        mixed[i] = total
        unit, _ = normalize(total)
        normed_two[rows_of(i, me), :] = (unit * norms_ref[2:3, :] + norms_ref[3:4, :]).astype(BF)
        gather_start(1, normed_two, i)

    def feed(i):
        gather_wait(1, normed_two, i)
        here = image_of(i)
        hidden = mm(normed_two[here, :], w_in[...]) + in_b_ref[...]
        square = hidden * hidden
        bent = jnp.tanh(ROOT * (hidden + CUBIC * (square * hidden)))
        half = 0.5 * (1.0 + bent)
        active[here, :] = (hidden * half).astype(BF)
        slope[here, :] = half + 0.5 * hidden * (1.0 - bent * bent) * (
            ROOT + (3.0 * CUBIC * ROOT) * square
        )
        sends[here, :] = mm(active[here, :], w_back[...]).astype(BF)
        part_start(1, i)

    def leave(i):
        out = mixed[i] + part_sum(1, i) + back_b_ref[...]

        @pl.when(section == 0)
        def _():
            passed[i] = out.astype(BF)
            pass_copy(0, i, tokens.at[i]).start()

        @pl.when(section == 1)
        def _():
            boundary_ref[i] = jnp.where(row_mask(i), out, 0.0)

    def grad_enter(i):
        @pl.when(section == 0)
        def _():
            pass_copy(1, i, grad_two.at[rows_of(i, me)]).wait_recv()
            gather_start(2, grad_two, i)

    def feed_back(i):
        gather_wait(2, grad_two, i)
        here = image_of(i)
        grad_active = mm(grad_two[here, :], w_back[...], 1, 1)
        held = (slope[here, :] * grad_active).astype(BF)
        grad_hidden[here, :] = held
        small_ref[6:7, :] += jnp.sum(held.astype(F32), axis=0, keepdims=True)
        sends[here, :] = mm(held, w_in[...], 1, 1).astype(BF)
        part_start(2, i)

    def middle_back(i):
        grad = part_sum(2, i)
        grad_y = grad_two[rows_of(i, me), :].astype(F32)
        grad_in, gain, offset = norm_backward(grad, mixed[i], norms_ref[2:3, :])
        total = grad_y + grad_in
        mixed[i] = total
        low = total.astype(BF)
        grad_one[rows_of(i, me), :] = low
        gather_start(3, grad_one, i)
        small_ref[2:3, :] += gain
        small_ref[3:4, :] += offset
        small_ref[4:5, :] += jnp.sum(low.astype(F32), axis=0, keepdims=True)
        small_ref[5:6, :] += jnp.sum(grad_y, axis=0, keepdims=True)

    def attend_back(i):
        gather_wait(3, grad_one, i)
        here = image_of(i)
        grad_heads = mm(grad_one[here, :], w_out[...], 1, 1).astype(BF)
        grad_heads = mm(grad_heads, selection(local, wide, head_size, False)).astype(BF)
        outs = ([], [], [])
        for h in range(heads):
            lanes = slice(h * LANES, (h + 1) * LANES)
            grad_out = grad_heads[:, lanes]
            prob = probs[i * heads + h]
            grad_prob = mm(grad_out, qkv[2, here, lanes], 1, 1)
            outs[2].append(mm(prob.astype(BF), grad_out, 0, 0).astype(BF))
            inner = jnp.sum(prob * grad_prob, axis=-1, keepdims=True)
            grad_scores = (prob * (grad_prob - inner)).astype(BF)
            score_sum[h, :, 0:seq] += grad_scores.astype(F32)
            outs[0].append((mm(grad_scores, qkv[1, here, lanes]) * score_scale).astype(BF))
            outs[1].append((mm(grad_scores, qkv[0, here, lanes], 0, 0) * score_scale).astype(BF))
        total = None
        chosen = selection(local, wide, head_size, True)
        for j in range(3):
            grad = jnp.concatenate(outs[j], axis=1)
            term = mm(grad, w_qkv[j], 1, 1)
            total = term if total is None else total + term
            grad_qkv[j, here, :] = mm(grad, chosen).astype(BF)
            if j != 1:
                columns_ref[i, j // 2 : j // 2 + 1, :] = jnp.sum(
                    grad.astype(F32), axis=0, keepdims=True
                )
        sends[here, :] = total.astype(BF)
        part_start(3, i)

    def grad_leave(i):
        grad = part_sum(3, i)
        grad_in, gain, offset = norm_backward(grad, tokens[i].astype(F32), norms_ref[0:1, :])
        total = mixed[i] + grad_in

        @pl.when(section == 1)
        def _():
            passed[i] = total.astype(BF)
            pass_copy(1, i, grad_two.at[rows_of(i, me)]).start()

        @pl.when(section == 0)
        def _():
            boundary_ref[i] = total

        small_ref[0:1, :] += gain
        small_ref[1:2, :] += offset

    def each(body):
        def step(i, carry):
            body(i)
            return carry

        lax.fori_loop(0, count, step, 0)

    @pl.when(section == 0)
    def _():
        copy = pltpu.make_async_copy(images_ref, tokens, load_sem.at[4])
        copy.start()
        copy.wait()
        each(enter)

    @pl.when(section == 1)
    def _():
        def given(i):
            low = jnp.where(row_mask(i), cotangent_ref[i].astype(F32), 0.0).astype(BF)
            grad_two[rows_of(i, me), :] = low
            gather_start(2, grad_two, i)

        each(given)

    small_ref[...] = jnp.zeros_like(small_ref)
    score_sum[...] = jnp.zeros_like(score_sum)
    for h in range(heads):
        spread = jnp.broadcast_to(table_ref[h : h + 1, :], (seq, 2 * seq))
        bias[h] = pltpu.roll(spread, seq + 1, 1, stride=1, stride_axis=0)[:, :seq]
    loads[0].wait()
    chosen = selection(local, wide, head_size, False)
    for j in range(3):
        w_qkv[j] = mm(w_raw[j], chosen).astype(BF)
    for load in loads[1:]:
        load.wait()

    def forward(i):
        @pl.when(section == 1)
        def _():
            enter(i)

        attend(i)
        middle(i)
        feed(i)
        leave(i)

    each(forward)

    def backward(i):
        grad_enter(i)
        feed_back(i)
        middle_back(i)
        attend_back(i)
        grad_leave(i)

    each(backward)

    @pl.when(section == 0)
    def _():
        each(lambda i: pass_copy(0, i, tokens.at[i]).wait_send())

    @pl.when(section == 1)
    def _():
        each(lambda i: pass_copy(1, i, grad_two.at[rows_of(i, me)]).wait_send())

    lanes = 2 * seq
    carried = [jnp.zeros((8, lanes), F32) for _ in range(heads)]
    fill = jnp.zeros((8, lanes - score_sum.shape[2]), F32)

    def shift_add(g, carried):
        where = pl.ds(pl.multiple_of(g * 8, 8), 8)
        return [
            pltpu.roll(c, 8, 1) + jnp.concatenate([score_sum[h, where, :], fill], axis=1)
            for h, c in enumerate(carried)
        ]

    carried = lax.fori_loop(0, seq // 8, shift_add, carried)
    behind = 7 - lax.broadcasted_iota(jnp.int32, (8, lanes), 0)
    for h in range(heads):
        c = carried[h]
        for by in (1, 2, 4):
            c = jnp.where((behind & by) != 0, pltpu.roll(c, by, 1), c)
        table_grad_ref[h : h + 1, :] = jnp.sum(c, axis=0, keepdims=True)

    jobs = [
        (grad_two, active, back_grad_ref, None),
        (normed_two, grad_hidden, in_grad_ref, None),
        (grad_one, mixed_heads, out_grad_ref, None),
    ] + [(normed, grad_qkv.at[j], qkv_grad_ref, j) for j in range(3)]
    tile = width // 3
    for left, right, dst, j in jobs:
        cols = right.shape[1]

        def tile_step(t, carry, left=left, right=right, cols=cols):
            where = pl.ds(pl.multiple_of(t * tile, LANES), tile)
            slope[where, 0:cols] = mm(left[:, where], right[...], 0, 0)
            return carry

        lax.fori_loop(0, 3, tile_step, 0)

        def store(s, carry, dst=dst, j=j, cols=cols):
            where = pl.ds(pl.multiple_of(s * share, 8), share)
            target = dst.at[s] if j is None else dst.at[s, j]
            spot = stage if cols == stage.shape[1] else thin_stage
            spot[...] = slope[where, 0:cols].astype(BF)
            copy = pltpu.make_async_copy(spot, target, store_sem)
            copy.start()
            copy.wait()
            return carry

        lax.fori_loop(0, shares, store, 0)


def run_layer(sizes, args):
    n, count, rows, width, hidden_width, heads, head_size, shares = sizes
    seq = n * rows
    local_width = heads * head_size
    wide = heads * LANES
    share = width // shares
    total = count * seq
    vmem = pl.BlockSpec(memory_space=pltpu.VMEM)
    anywhere = pl.BlockSpec(memory_space=pl.ANY)
    dma = pltpu.SemaphoreType.DMA
    return pl.pallas_call(
        functools.partial(layer_kernel, sizes),
        out_shape=(
            jax.ShapeDtypeStruct((count, rows, width), F32),
            jax.ShapeDtypeStruct((8, width), F32),
            jax.ShapeDtypeStruct((heads, 2 * seq), F32),
            jax.ShapeDtypeStruct((count, 2, wide), F32),
            jax.ShapeDtypeStruct((shares, 3, share, local_width), BF),
            jax.ShapeDtypeStruct((shares, share, local_width), BF),
            jax.ShapeDtypeStruct((shares, share, hidden_width), BF),
            jax.ShapeDtypeStruct((shares, share, hidden_width), BF),
        ),
        in_specs=[
            pl.BlockSpec(memory_space=pltpu.SMEM),
            anywhere,
            vmem,
            vmem,
            vmem,
            anywhere,
            anywhere,
            vmem,
            anywhere,
            vmem,
            anywhere,
            vmem,
            vmem,
        ],
        out_specs=(vmem, vmem, vmem, vmem, anywhere, anywhere, anywhere, anywhere),
        scratch_shapes=[
            pltpu.VMEM((3, width, local_width), BF),
            pltpu.VMEM((3, width, wide), BF),
            pltpu.VMEM((local_width, width), BF),
            pltpu.VMEM((width, hidden_width), BF),
            pltpu.VMEM((hidden_width, width), BF),
            pltpu.VMEM((total, width), BF),
            pltpu.VMEM((total, width), BF),
            pltpu.VMEM((total, width), BF),
            pltpu.VMEM((total, width), BF),
            pltpu.VMEM((total, hidden_width), BF),
            pltpu.VMEM((total, hidden_width), BF),
            pltpu.VMEM((3, total, wide), BF),
            pltpu.VMEM((total, local_width), BF),
            pltpu.VMEM((3, total, local_width), BF),
            pltpu.VMEM((count * heads, seq, seq), F32),
            pltpu.VMEM((max(total, width), hidden_width), F32),
            pltpu.VMEM((heads, seq, seq), F32),
            pltpu.VMEM((heads, seq, -(-seq // LANES) * LANES), F32),
            pltpu.VMEM((2, count, n - 1, rows, width), BF),
            pltpu.VMEM((total, width), BF),
            pltpu.VMEM((count, rows, width), BF),
            pltpu.VMEM((count, rows, width), BF),
            pltpu.VMEM((count, rows, width), F32),
            pltpu.VMEM((share, hidden_width), BF),
            pltpu.VMEM((share, local_width), BF),
            dma((5,)),
            dma((4, count, n - 1)),
            dma((4, count, n - 1)),
            dma((4, count, n - 1)),
            dma((4, count, n - 1)),
            dma((2, count)),
            dma((2, count)),
            dma,
        ],
        compiler_params=pltpu.CompilerParams(
            collective_id=0, has_side_effects=True, vmem_limit_bytes=67043328
        ),
        name="two_pass",
    )(*args)


def local(
    images,
    cotangent,
    lengths,
    timesteps,
    time_table,
    norms,
    qkv_weight,
    time_weight,
    out_weight,
    out_bias,
    mlp_in_weight,
    mlp_in_bias,
    mlp_out_weight,
    mlp_out_bias,
    rel_bias,
):
    count, rows, width = images.shape
    local_width = qkv_weight.shape[3]
    hidden_width = mlp_in_weight.shape[2]
    heads = rel_bias.shape[1]
    head_size = local_width // heads
    shares = lax.axis_size("dp")
    share = width // shares
    sizes = (lax.axis_size("mp"), count, rows, width, hidden_width, heads, head_size, shares)
    time_rows = jnp.concatenate(
        [lax.dynamic_slice_in_dim(time_table, timesteps[i], 1, axis=0) for i in range(count)]
    )
    time_part = jnp.dot(
        time_rows, time_weight[0].reshape(width, 2 * local_width), preferred_element_type=F32
    ).reshape(count, 2, heads, head_size)
    time_part = jnp.pad(time_part, ((0, 0), (0, 0), (0, 0), (0, LANES - head_size)))
    time_part = time_part.reshape(count, 2, heads * LANES)
    table = jnp.pad(jnp.flip(rel_bias[0], axis=1), ((0, 0), (0, 1)))
    outs = run_layer(
        sizes,
        (
            lengths,
            images,
            cotangent,
            time_part,
            norms[0],
            jnp.transpose(qkv_weight[0], (1, 0, 2)),
            out_weight[0],
            out_bias,
            mlp_in_weight[0],
            mlp_in_bias,
            mlp_out_weight[0],
            mlp_out_bias,
            table,
        ),
    )
    boundary, small, table_grad, columns, qkv_grad, out_grad, in_grad, back_grad = outs
    columns = columns.reshape(count, 2, heads, LANES)[..., :head_size]
    columns = columns.reshape(count, 2 * local_width)
    all_columns = lax.all_gather(columns, "dp", axis=0, tiled=True)
    all_steps = lax.all_gather(timesteps, "dp", axis=0, tiled=True)
    all_rows = lax.dynamic_slice_in_dim(
        time_table[all_steps], lax.axis_index("dp") * share, share, axis=1
    )
    time_grad = lax.dot_general(
        all_rows.astype(F32),
        all_columns,
        (((0,), (0,)), ((), ())),
        precision=lax.Precision.HIGHEST,
        preferred_element_type=F32,
    ).reshape(share, 2, local_width)

    def scatter(value):
        return lax.psum_scatter(value, "dp", scatter_dimension=0).astype(F32)

    table_sum = lax.psum((jnp.flip(table_grad[:, : rel_bias.shape[2]], axis=1), small[6]), "dp")
    shared = lax.psum(small[:6], ("dp", "mp"))
    return (
        boundary[None],
        shared[None, :4],
        jnp.transpose(scatter(qkv_grad), (1, 0, 2))[None],
        time_grad[None],
        scatter(out_grad).T[None],
        shared[4][None],
        scatter(in_grad)[None],
        table_sum[1][None],
        scatter(back_grad).T[None],
        shared[5][None],
        table_sum[0][None],
    )


def solution(mesh):
    in_specs = (
        P("dp", "mp", None),
        P("dp", "mp", None),
        P("dp"),
        P("dp"),
        P(),
        P("section", None, None),
        P("section", None, None, "mp"),
        P("section", None, None, "mp"),
        P("section", "mp", None),
        P("section", None),
        P("section", None, "mp"),
        P("section", "mp"),
        P("section", "mp", None),
        P("section", None),
        P("section", "mp", None),
    )
    out_specs = (
        P("section", "dp", "mp", None),
        P("section", None, None),
        P("section", "dp", None, "mp"),
        P("section", "dp", None, "mp"),
        P("section", "mp", "dp"),
        P("section", None),
        P("section", "dp", "mp"),
        P("section", "mp"),
        P("section", "mp", "dp"),
        P("section", None),
        P("section", "mp", None),
    )
    return jax.shard_map(local, mesh=mesh, in_specs=in_specs, out_specs=out_specs, check_vma=False)
```

```python
import functools
import math

import jax
import jax.numpy as jnp
from jax import lax
from jax.experimental import pallas as pl
from jax.experimental.pallas import tpu as pltpu
from jax.sharding import PartitionSpec as P

EPSILON = 1e-06
NEG_FILL = -1000000000.0
LANES = 128
BF = jnp.bfloat16
F32 = jnp.float32
ROOT = math.sqrt(2.0 / math.pi)
CUBIC = 0.044715


def mm(left, right, left_dim=1, right_dim=0):
    return lax.dot_general(
        left, right, (((left_dim,), (right_dim,)), ((), ())), preferred_element_type=F32
    )


def selection(rows, cols, head_size, flip):
    shape = (cols, rows) if flip else (rows, cols)
    row = lax.broadcasted_iota(jnp.int32, shape, 1 if flip else 0)
    col = lax.broadcasted_iota(jnp.int32, shape, 0 if flip else 1)
    within = col & (LANES - 1)
    hit = (within < head_size) & (row == (col // LANES) * head_size + within)
    return jnp.where(hit, 1.0, 0.0).astype(BF)


def normalize(values):
    centred = values - jnp.mean(values, axis=-1, keepdims=True)
    spread = jnp.mean(centred * centred, axis=-1, keepdims=True)
    scale = lax.rsqrt(spread + EPSILON)
    return centred * scale, scale


def norm_backward(grad, values, gain):
    unit, scale = normalize(values)
    inner = grad * gain
    mean_one = jnp.mean(inner, axis=-1, keepdims=True)
    mean_two = jnp.mean(inner * unit, axis=-1, keepdims=True)
    grad_in = scale * (inner - mean_one - unit * mean_two)
    gain_grad = jnp.sum(grad * unit, axis=0, keepdims=True)
    offset_grad = jnp.sum(grad, axis=0, keepdims=True)
    return grad_in, gain_grad, offset_grad


def layer_kernel(
    sizes,
    lengths_ref,
    images_ref,
    cotangent_ref,
    time_ref,
    norms_ref,
    qkv_raw_ref,
    out_w_ref,
    out_b_ref,
    in_w_ref,
    in_b_ref,
    back_w_ref,
    back_b_ref,
    table_ref,
    steps_ref,
    boundary_ref,
    small_ref,
    table_grad_ref,
    columns_ref,
    rows_ref,
    qkv_grad_ref,
    out_grad_ref,
    in_grad_ref,
    back_grad_ref,
    w_raw,
    w_qkv,
    w_out,
    w_in,
    w_back,
    normed,
    normed_two,
    grad_two,
    grad_one,
    active,
    grad_hidden,
    qkv,
    mixed_heads,
    grad_qkv,
    probs,
    slope,
    bias,
    score_sum,
    parts,
    sends,
    tokens,
    passed,
    mixed,
    thin,
    sums,
    all_sums,
    load_sem,
    gather_send,
    gather_recv,
    part_send,
    part_recv,
    pass_send,
    pass_recv,
    weight_send,
    weight_recv,
    weight_own,
    tiny_send,
    tiny_recv,
    sum_send,
    sum_recv,
):
    n, count, rows, width, hidden_width, heads, head_size, shares = sizes
    seq = n * rows
    local = heads * head_size
    wide = heads * LANES
    share = width // shares
    score_scale = 1.0 / math.sqrt(head_size)
    me = lax.axis_index("mp")
    section = lax.axis_index("section")
    replica = lax.axis_index("dp")
    own = pl.multiple_of(me * rows, 16)

    def peer(d):
        return lax.rem(me + d, n)

    def source(d):
        return lax.rem(me + n - d, n)

    barrier = pltpu.get_barrier_semaphore()
    for d in range(1, n):
        pl.semaphore_signal(barrier, inc=1, device_id={"mp": peer(d)})
    pl.semaphore_signal(barrier, inc=1, device_id={"section": 1 - section})
    for d in range(1, shares):
        pl.semaphore_signal(barrier, inc=1, device_id={"dp": lax.rem(replica + d, shares)})
    pl.semaphore_wait(barrier, n + shares - 1)

    loads = [
        pltpu.make_async_copy(a, b, load_sem.at[k])
        for k, (a, b) in enumerate(
            [(qkv_raw_ref, w_raw), (out_w_ref, w_out), (in_w_ref, w_in), (back_w_ref, w_back)]
        )
    ]
    for load in loads:
        load.start()

    def rows_of(i, index):
        return pl.ds(pl.multiple_of(i * seq + index * rows, 16), rows)

    def image_of(i):
        return pl.ds(pl.multiple_of(i * seq, 16), seq)

    def gather_copy(kind, buf, i, d, index):
        where = rows_of(i, index)
        return pltpu.make_async_remote_copy(
            src_ref=buf.at[where],
            dst_ref=buf.at[where],
            send_sem=gather_send.at[kind, i, d - 1],
            recv_sem=gather_recv.at[kind, i, d - 1],
            device_id={"mp": peer(d)},
        )

    def gather_start(kind, buf, i):
        for d in range(1, n):
            gather_copy(kind, buf, i, d, me).start()

    def gather_wait(kind, buf, i):
        for d in range(1, n):
            gather_copy(kind, buf, i, d, me).wait_send()
            gather_copy(kind, buf, i, d, source(d)).wait_recv()

    def part_copy(kind, i, d):
        return pltpu.make_async_remote_copy(
            src_ref=sends.at[rows_of(i, peer(d))],
            dst_ref=parts.at[kind & 1, i, d - 1],
            send_sem=part_send.at[kind, i, d - 1],
            recv_sem=part_recv.at[kind, i, d - 1],
            device_id={"mp": peer(d)},
        )

    def part_start(kind, i):
        for d in range(1, n):
            part_copy(kind, i, d).start()

    def part_sum(kind, i):
        for d in range(1, n):
            part_copy(kind, i, d).wait()
        total = sends[rows_of(i, me), :].astype(F32)
        for d in range(1, n):
            total = total + parts[kind & 1, i, d - 1].astype(F32)
        return total

    def pass_copy(k, i, dst):
        return pltpu.make_async_remote_copy(
            src_ref=passed.at[i],
            dst_ref=dst,
            send_sem=pass_send.at[k, i],
            recv_sem=pass_recv.at[k, i],
            device_id={"section": 1 - section},
        )

    def row_mask(i):
        index = me * rows + lax.broadcasted_iota(jnp.int32, (rows, 1), 0)
        return index < lengths_ref[i]

    def enter(i):
        @pl.when(section == 1)
        def _():
            pass_copy(0, i, tokens.at[i]).wait_recv()

        unit, _ = normalize(tokens[i].astype(F32))
        normed[rows_of(i, me), :] = (unit * norms_ref[0:1, :] + norms_ref[1:2, :]).astype(BF)
        gather_start(0, normed, i)

    def attend(i):
        gather_wait(0, normed, i)
        here = image_of(i)
        for j in range(3):
            linear = mm(normed[here, :], w_qkv[j])
            if j == 0:
                linear = linear + time_ref[i, 0:1, :]
            if j == 2:
                linear = linear + time_ref[i, 1:2, :]
            qkv[j, here, :] = linear.astype(BF)
        key_index = lax.broadcasted_iota(jnp.int32, (1, seq), 1)
        key_mask = key_index < lengths_ref[i]
        outs = []
        for h in range(heads):
            lanes = slice(h * LANES, (h + 1) * LANES)
            scores = mm(qkv[0, here, lanes], qkv[1, here, lanes], 1, 1) * score_scale + bias[h]
            scores = jnp.where(key_mask, scores, NEG_FILL)
            top = jnp.max(scores, axis=-1, keepdims=True)
            raised = jnp.exp(scores - top)
            prob = raised / jnp.sum(raised, axis=-1, keepdims=True)
            probs[i * heads + h] = prob
            outs.append(mm(prob.astype(BF), qkv[2, here, lanes]).astype(BF))
        packed = mm(jnp.concatenate(outs, axis=1), selection(local, wide, head_size, True))
        packed = packed.astype(BF)
        mixed_heads[here, :] = packed
        sends[here, :] = mm(packed, w_out[...]).astype(BF)
        part_start(0, i)

    def middle(i):
        total = tokens[i].astype(F32) + part_sum(0, i) + out_b_ref[...]
        mixed[i] = total
        unit, _ = normalize(total)
        normed_two[rows_of(i, me), :] = (unit * norms_ref[2:3, :] + norms_ref[3:4, :]).astype(BF)
        gather_start(1, normed_two, i)

    def feed(i):
        gather_wait(1, normed_two, i)
        here = image_of(i)
        hidden = mm(normed_two[here, :], w_in[...]) + in_b_ref[...]
        square = hidden * hidden
        bent = jnp.tanh(ROOT * (hidden + CUBIC * (square * hidden)))
        half = 0.5 * (1.0 + bent)
        active[here, :] = (hidden * half).astype(BF)
        slope[here, :] = half + 0.5 * hidden * (1.0 - bent * bent) * (
            ROOT + (3.0 * CUBIC * ROOT) * square
        )
        sends[here, :] = mm(active[here, :], w_back[...]).astype(BF)
        part_start(1, i)

    def leave(i):
        out = mixed[i] + part_sum(1, i) + back_b_ref[...]

        @pl.when(section == 0)
        def _():
            passed[i] = out.astype(BF)
            pass_copy(0, i, tokens.at[i]).start()

        @pl.when(section == 1)
        def _():
            boundary_ref[i] = jnp.where(row_mask(i), out, 0.0)

    def grad_enter(i):
        @pl.when(section == 0)
        def _():
            pass_copy(1, i, grad_two.at[rows_of(i, me)]).wait_recv()
            gather_start(2, grad_two, i)

    def feed_back(i):
        gather_wait(2, grad_two, i)
        here = image_of(i)
        grad_active = mm(grad_two[here, :], w_back[...], 1, 1)
        held = (slope[here, :] * grad_active).astype(BF)
        grad_hidden[here, :] = held
        sums[6:7, :] += jnp.sum(held.astype(F32), axis=0, keepdims=True)
        sends[here, :] = mm(held, w_in[...], 1, 1).astype(BF)
        part_start(2, i)

    def middle_back(i):
        grad = part_sum(2, i)
        grad_y = grad_two[rows_of(i, me), :].astype(F32)
        grad_in, gain, offset = norm_backward(grad, mixed[i], norms_ref[2:3, :])
        total = grad_y + grad_in
        mixed[i] = total
        low = total.astype(BF)
        grad_one[rows_of(i, me), :] = low
        gather_start(3, grad_one, i)
        sums[2:3, :] += gain
        sums[3:4, :] += offset
        sums[4:5, :] += jnp.sum(low.astype(F32), axis=0, keepdims=True)
        sums[5:6, :] += jnp.sum(grad_y, axis=0, keepdims=True)

    def attend_back(i):
        gather_wait(3, grad_one, i)
        here = image_of(i)
        grad_heads = mm(grad_one[here, :], w_out[...], 1, 1).astype(BF)
        grad_heads = mm(grad_heads, selection(local, wide, head_size, False)).astype(BF)
        outs = ([], [], [])
        for h in range(heads):
            lanes = slice(h * LANES, (h + 1) * LANES)
            grad_out = grad_heads[:, lanes]
            prob = probs[i * heads + h]
            grad_prob = mm(grad_out, qkv[2, here, lanes], 1, 1)
            outs[2].append(mm(prob.astype(BF), grad_out, 0, 0).astype(BF))
            inner = jnp.sum(prob * grad_prob, axis=-1, keepdims=True)
            grad_scores = (prob * (grad_prob - inner)).astype(BF)
            score_sum[h, :, 0:seq] += grad_scores.astype(F32)
            outs[0].append((mm(grad_scores, qkv[1, here, lanes]) * score_scale).astype(BF))
            outs[1].append((mm(grad_scores, qkv[0, here, lanes], 0, 0) * score_scale).astype(BF))
        total = None
        chosen = selection(local, wide, head_size, True)
        for j in range(3):
            grad = jnp.concatenate(outs[j], axis=1)
            term = mm(grad, w_qkv[j], 1, 1)
            total = term if total is None else total + term
            grad_qkv[j, here, :] = mm(grad, chosen).astype(BF)
            if j != 1:
                columns_ref[replica, i, j // 2 : j // 2 + 1, :] = jnp.sum(
                    grad.astype(F32), axis=0, keepdims=True
                )
        sends[here, :] = total.astype(BF)
        part_start(3, i)

    def grad_leave(i):
        grad = part_sum(3, i)
        grad_in, gain, offset = norm_backward(grad, tokens[i].astype(F32), norms_ref[0:1, :])
        total = mixed[i] + grad_in

        @pl.when(section == 1)
        def _():
            passed[i] = total.astype(BF)
            pass_copy(1, i, grad_two.at[rows_of(i, me)]).start()

        @pl.when(section == 0)
        def _():
            boundary_ref[i] = total

        sums[0:1, :] += gain
        sums[1:2, :] += offset

    def each(body):
        def step(i, carry):
            body(i)
            return carry

        lax.fori_loop(0, count, step, 0)

    @pl.when(section == 0)
    def _():
        copy = pltpu.make_async_copy(images_ref, tokens, load_sem.at[4])
        copy.start()
        copy.wait()
        each(enter)

    @pl.when(section == 1)
    def _():
        def given(i):
            low = jnp.where(row_mask(i), cotangent_ref[i].astype(F32), 0.0).astype(BF)
            grad_two[rows_of(i, me), :] = low
            gather_start(2, grad_two, i)

        each(given)

    sums[...] = jnp.zeros_like(sums)
    score_sum[...] = jnp.zeros_like(score_sum)
    for h in range(heads):
        spread = jnp.broadcast_to(table_ref[h : h + 1, :], (seq, 2 * seq))
        bias[h] = pltpu.roll(spread, seq + 1, 1, stride=1, stride_axis=0)[:, :seq]
    loads[0].wait()
    chosen = selection(local, wide, head_size, False)
    for j in range(3):
        w_qkv[j] = mm(w_raw[j], chosen).astype(BF)
    for load in loads[1:]:
        load.wait()

    def replica_peer(d):
        return lax.rem(replica + d, shares)

    def replica_source(d):
        return lax.rem(replica + shares - d, shares)

    def share_of(index):
        return pl.ds(pl.multiple_of(index * share, 8), share)

    def slot(array, index, j):
        return array.at[index] if j is None else array.at[index, j]

    jobs = [
        (grad_two, active, w_back, back_grad_ref, None),
        (normed_two, grad_hidden, w_in, in_grad_ref, None),
        (grad_one, mixed_heads, thin, out_grad_ref, None),
    ] + [(normed, grad_qkv.at[j], w_raw.at[j], qkv_grad_ref, j) for j in range(3)]
    tile = width // 3

    def own_copy(k):
        _, _, buf, dst, j = jobs[k]
        return pltpu.make_async_copy(
            buf.at[share_of(replica)], slot(dst, replica, j), weight_own.at[k]
        )

    def weight_copy(k, d, index):
        _, _, buf, dst, j = jobs[k]
        return pltpu.make_async_remote_copy(
            src_ref=buf.at[share_of(replica_peer(d))],
            dst_ref=slot(dst, index, j),
            send_sem=weight_send.at[k, d - 1],
            recv_sem=weight_recv.at[k, d - 1],
            device_id={"dp": replica_peer(d)},
        )

    def weight_job(k):
        left, right, buf, _, _ = jobs[k]

        def tile_step(t, carry):
            where = pl.ds(pl.multiple_of(t * tile, LANES), tile)
            buf[where, :] = mm(left[:, where], right[...], 0, 0).astype(BF)
            return carry

        lax.fori_loop(0, 3, tile_step, 0)
        own_copy(k).start()
        for d in range(1, shares):
            weight_copy(k, d, replica).start()

    def qkv_jobs(i):
        for k in range(3, 6):
            weight_job(k)

    def later_enter(i):
        @pl.when(section == 1)
        def _():
            enter(i)

    schedule = (
        (grad_enter, 11, 14, count),
        (attend, 2, 2, count),
        (middle, 3, 3, count),
        (later_enter, 0, 0, count),
        (leave, 6, 10, count),
        (feed_back, 15, 10, count),
        (grad_leave, 31, 17, count),
        (feed, 4, 7, count),
        (lambda i: weight_job(2), 31, 17, 1),
        (qkv_jobs, 30, 19, 1),
        (lambda i: weight_job(1), 17, 18, 1),
        (middle_back, 23, 12, count),
        (attend_back, 26, 14, count),
        (lambda i: weight_job(0), 24, 19, 1),
    )
    steps = max(max(first, second) for _, first, second, _ in schedule) + count

    def tick(t, carry):
        for body, first, second, times in schedule:
            i = t - (first + section * (second - first))

            @pl.when((i >= 0) & (i < times))
            def _(body=body, i=i):
                body(i)

        return carry

    lax.fori_loop(0, steps, tick, 0)

    @pl.when(section == 0)
    def _():
        each(lambda i: pass_copy(0, i, tokens.at[i]).wait_send())

    @pl.when(section == 1)
    def _():
        each(lambda i: pass_copy(1, i, grad_two.at[rows_of(i, me)]).wait_send())

    def sum_copy(d, index):
        return pltpu.make_async_remote_copy(
            src_ref=all_sums.at[me],
            dst_ref=all_sums.at[index],
            send_sem=sum_send.at[d - 1],
            recv_sem=sum_recv.at[d - 1],
            device_id={"mp": peer(d)},
        )

    all_sums[me] = sums[...]
    for d in range(1, n):
        sum_copy(d, me).start()

    lanes = 2 * seq
    carried = [jnp.zeros((8, lanes), F32) for _ in range(heads)]
    fill = jnp.zeros((8, lanes - score_sum.shape[2]), F32)

    def shift_add(g, carried):
        where = pl.ds(pl.multiple_of(g * 8, 8), 8)
        return [
            pltpu.roll(c, 8, 1) + jnp.concatenate([score_sum[h, where, :], fill], axis=1)
            for h, c in enumerate(carried)
        ]

    carried = lax.fori_loop(0, seq // 8, shift_add, carried)
    behind = 7 - lax.broadcasted_iota(jnp.int32, (8, lanes), 0)
    for h in range(heads):
        c = carried[h]
        for by in (1, 2, 4):
            c = jnp.where((behind & by) != 0, pltpu.roll(c, by, 1), c)
        table_grad_ref[replica, h : h + 1, :] = jnp.sum(c, axis=0, keepdims=True)

    for d in range(1, n):
        sum_copy(d, me).wait_send()
        sum_copy(d, source(d)).wait_recv()
    total = all_sums[0]
    for k in range(1, n):
        total = total + all_sums[k]
    kind = lax.broadcasted_iota(jnp.int32, (8, width), 0)
    small_ref[replica] = jnp.where(kind < 6, total, sums[...])

    tiny = (small_ref, table_grad_ref, columns_ref, rows_ref)

    def tiny_copy(k, d, index):
        return pltpu.make_async_remote_copy(
            src_ref=tiny[k].at[replica],
            dst_ref=tiny[k].at[index],
            send_sem=tiny_send.at[k, d - 1],
            recv_sem=tiny_recv.at[k, d - 1],
            device_id={"dp": replica_peer(d)},
        )

    rows_ref[replica] = steps_ref[...]
    for k in range(4):
        for d in range(1, shares):
            tiny_copy(k, d, replica).start()
    for k in range(6):
        own_copy(k).wait()
        for d in range(1, shares):
            weight_copy(k, d, replica).wait_send()
            weight_copy(k, d, replica_source(d)).wait_recv()
    for k in range(4):
        for d in range(1, shares):
            tiny_copy(k, d, replica).wait_send()
            tiny_copy(k, d, replica_source(d)).wait_recv()


def run_layer(sizes, args):
    n, count, rows, width, hidden_width, heads, head_size, shares = sizes
    seq = n * rows
    local_width = heads * head_size
    wide = heads * LANES
    share = width // shares
    total = count * seq
    vmem = pl.BlockSpec(memory_space=pltpu.VMEM)
    anywhere = pl.BlockSpec(memory_space=pl.ANY)
    dma = pltpu.SemaphoreType.DMA
    return pl.pallas_call(
        functools.partial(layer_kernel, sizes),
        out_shape=(
            jax.ShapeDtypeStruct((count, rows, width), F32),
            jax.ShapeDtypeStruct((shares, 8, width), F32),
            jax.ShapeDtypeStruct((shares, heads, 2 * seq), F32),
            jax.ShapeDtypeStruct((shares, count, 2, wide), F32),
            jax.ShapeDtypeStruct((shares, count, width), BF),
            jax.ShapeDtypeStruct((shares, 3, share, local_width), BF),
            jax.ShapeDtypeStruct((shares, share, local_width), BF),
            jax.ShapeDtypeStruct((shares, share, hidden_width), BF),
            jax.ShapeDtypeStruct((shares, share, hidden_width), BF),
        ),
        in_specs=[
            pl.BlockSpec(memory_space=pltpu.SMEM),
            anywhere,
            vmem,
            vmem,
            vmem,
            anywhere,
            anywhere,
            vmem,
            anywhere,
            vmem,
            anywhere,
            vmem,
            vmem,
            vmem,
        ],
        out_specs=(vmem, vmem, vmem, vmem, vmem, anywhere, anywhere, anywhere, anywhere),
        scratch_shapes=[
            pltpu.VMEM((3, width, local_width), BF),
            pltpu.VMEM((3, width, wide), BF),
            pltpu.VMEM((local_width, width), BF),
            pltpu.VMEM((width, hidden_width), BF),
            pltpu.VMEM((hidden_width, width), BF),
            pltpu.VMEM((total, width), BF),
            pltpu.VMEM((total, width), BF),
            pltpu.VMEM((total, width), BF),
            pltpu.VMEM((total, width), BF),
            pltpu.VMEM((total, hidden_width), BF),
            pltpu.VMEM((total, hidden_width), BF),
            pltpu.VMEM((3, total, wide), BF),
            pltpu.VMEM((total, local_width), BF),
            pltpu.VMEM((3, total, local_width), BF),
            pltpu.VMEM((count * heads, seq, seq), F32),
            pltpu.VMEM((total, hidden_width), F32),
            pltpu.VMEM((heads, seq, seq), F32),
            pltpu.VMEM((heads, seq, -(-seq // LANES) * LANES), F32),
            pltpu.VMEM((2, count, n - 1, rows, width), BF),
            pltpu.VMEM((total, width), BF),
            pltpu.VMEM((count, rows, width), BF),
            pltpu.VMEM((count, rows, width), BF),
            pltpu.VMEM((count, rows, width), F32),
            pltpu.VMEM((width, local_width), BF),
            pltpu.VMEM((8, width), F32),
            pltpu.VMEM((n, 8, width), F32),
            dma((5,)),
            dma((4, count, n - 1)),
            dma((4, count, n - 1)),
            dma((4, count, n - 1)),
            dma((4, count, n - 1)),
            dma((2, count)),
            dma((2, count)),
            dma((6, shares - 1)),
            dma((6, shares - 1)),
            dma((6,)),
            dma((4, shares - 1)),
            dma((4, shares - 1)),
            dma((n - 1,)),
            dma((n - 1,)),
        ],
        compiler_params=pltpu.CompilerParams(
            collective_id=0, has_side_effects=True, vmem_limit_bytes=67043328
        ),
        name="two_pass",
    )(*args)


def local(
    images,
    cotangent,
    lengths,
    timesteps,
    time_table,
    norms,
    qkv_weight,
    time_weight,
    out_weight,
    out_bias,
    mlp_in_weight,
    mlp_in_bias,
    mlp_out_weight,
    mlp_out_bias,
    rel_bias,
):
    count, rows, width = images.shape
    local_width = qkv_weight.shape[3]
    hidden_width = mlp_in_weight.shape[2]
    heads = rel_bias.shape[1]
    head_size = local_width // heads
    shares = lax.axis_size("dp")
    share = width // shares
    sizes = (lax.axis_size("mp"), count, rows, width, hidden_width, heads, head_size, shares)
    time_rows = jnp.concatenate(
        [lax.dynamic_slice_in_dim(time_table, timesteps[i], 1, axis=0) for i in range(count)]
    )
    time_part = jnp.dot(
        time_rows, time_weight[0].reshape(width, 2 * local_width), preferred_element_type=F32
    ).reshape(count, 2, heads, head_size)
    time_part = jnp.pad(time_part, ((0, 0), (0, 0), (0, 0), (0, LANES - head_size)))
    time_part = time_part.reshape(count, 2, heads * LANES)
    table = jnp.pad(jnp.flip(rel_bias[0], axis=1), ((0, 0), (0, 1)))
    outs = run_layer(
        sizes,
        (
            lengths,
            images,
            cotangent,
            time_part,
            norms[0],
            jnp.transpose(qkv_weight[0], (1, 0, 2)),
            out_weight[0],
            out_bias,
            mlp_in_weight[0],
            mlp_in_bias,
            mlp_out_weight[0],
            mlp_out_bias,
            table,
            time_rows,
        ),
    )
    boundary, small, table_grad, columns, all_rows, qkv_grad, out_grad, in_grad, back_grad = outs
    columns = columns.reshape(shares * count, 2, heads, LANES)[..., :head_size]
    columns = columns.reshape(shares * count, 2 * local_width)
    all_rows = lax.dynamic_slice_in_dim(
        all_rows.reshape(shares * count, width), lax.axis_index("dp") * share, share, axis=1
    )
    time_grad = lax.dot_general(
        all_rows.astype(F32),
        columns,
        (((0,), (0,)), ((), ())),
        precision=lax.Precision.HIGHEST,
        preferred_element_type=F32,
    ).reshape(share, 2, local_width)

    def added(value):
        return jnp.sum(value.astype(F32), axis=0)

    small = added(small)
    table_grad = jnp.flip(added(table_grad)[:, : rel_bias.shape[2]], axis=1)
    return (
        boundary[None],
        small[None, :4],
        jnp.transpose(added(qkv_grad), (1, 0, 2))[None],
        time_grad[None],
        added(out_grad).T[None],
        small[4][None],
        added(in_grad)[None],
        small[6][None],
        added(back_grad).T[None],
        small[5][None],
        table_grad[None],
    )


def solution(mesh):
    in_specs = (
        P("dp", "mp", None),
        P("dp", "mp", None),
        P("dp"),
        P("dp"),
        P(),
        P("section", None, None),
        P("section", None, None, "mp"),
        P("section", None, None, "mp"),
        P("section", "mp", None),
        P("section", None),
        P("section", None, "mp"),
        P("section", "mp"),
        P("section", "mp", None),
        P("section", None),
        P("section", "mp", None),
    )
    out_specs = (
        P("section", "dp", "mp", None),
        P("section", None, None),
        P("section", "dp", None, "mp"),
        P("section", "dp", None, "mp"),
        P("section", "mp", "dp"),
        P("section", None),
        P("section", "dp", "mp"),
        P("section", "mp"),
        P("section", "mp", "dp"),
        P("section", None),
        P("section", "mp", None),
    )
    return jax.shard_map(local, mesh=mesh, in_specs=in_specs, out_specs=out_specs, check_vma=False)
```

```python
import functools
import math

import jax
import jax.numpy as jnp
from jax import lax
from jax.experimental import pallas as pl
from jax.experimental.pallas import tpu as pltpu
from jax.sharding import PartitionSpec as P

EPSILON = 1e-06
NEG_FILL = -1000000000.0
LANES = 128
BF = jnp.bfloat16
F32 = jnp.float32
ROOT = math.sqrt(2.0 / math.pi)
CUBIC = 0.044715


def mm(left, right, left_dim=1, right_dim=0):
    return lax.dot_general(
        left, right, (((left_dim,), (right_dim,)), ((), ())), preferred_element_type=F32
    )


def selection(rows, cols, head_size, flip, first=0):
    shape = (cols, rows) if flip else (rows, cols)
    row = lax.broadcasted_iota(jnp.int32, shape, 1 if flip else 0)
    col = lax.broadcasted_iota(jnp.int32, shape, 0 if flip else 1)
    within = col & (LANES - 1)
    hit = (within < head_size) & (row - first == (col // LANES) * head_size + within)
    return jnp.where(hit, 1.0, 0.0).astype(BF)


def normalize(values):
    centred = values - jnp.mean(values, axis=-1, keepdims=True)
    spread = jnp.mean(centred * centred, axis=-1, keepdims=True)
    scale = lax.rsqrt(spread + EPSILON)
    return centred * scale, scale


def norm_backward(grad, values, gain):
    unit, scale = normalize(values)
    inner = grad * gain
    mean_one = jnp.mean(inner, axis=-1, keepdims=True)
    mean_two = jnp.mean(inner * unit, axis=-1, keepdims=True)
    grad_in = scale * (inner - mean_one - unit * mean_two)
    gain_grad = jnp.sum(grad * unit, axis=0, keepdims=True)
    offset_grad = jnp.sum(grad, axis=0, keepdims=True)
    return grad_in, gain_grad, offset_grad


def layer_kernel(
    sizes,
    lengths_ref,
    images_ref,
    cotangent_ref,
    time_ref,
    norms_ref,
    qkv_raw_ref,
    out_w_ref,
    out_b_ref,
    in_w_ref,
    in_b_ref,
    back_w_ref,
    back_b_ref,
    table_ref,
    steps_ref,
    boundary_ref,
    small_ref,
    table_grad_ref,
    columns_ref,
    rows_ref,
    thin_grad_ref,
    in_grad_ref,
    back_grad_ref,
    w_raw,
    w_qkv,
    w_out,
    w_in,
    w_back,
    normed,
    normed_two,
    grad_two,
    grad_one,
    active,
    grad_hidden,
    qkv,
    mixed_heads,
    grad_qkv,
    probs,
    slope,
    bias,
    score_sum,
    parts,
    sends,
    tokens,
    passed,
    mixed,
    crossed,
    sums,
    all_sums,
    load_sem,
    gather_send,
    gather_recv,
    part_send,
    part_recv,
    pass_send,
    pass_recv,
    weight_send,
    weight_recv,
    weight_own,
    tiny_send,
    tiny_recv,
    sum_send,
    sum_recv,
):
    n, count, rows, width, hidden_width, heads, head_size, shares = sizes
    seq = n * rows
    local = heads * head_size
    wide = heads * LANES
    share = width // shares
    score_scale = 1.0 / math.sqrt(head_size)
    me = lax.axis_index("mp")
    section = lax.axis_index("section")
    replica = lax.axis_index("dp")
    own = pl.multiple_of(me * rows, 16)

    def peer(d):
        if n == 4:
            return (n - 1 - me, me + 1 - 2 * lax.rem(me, 2), lax.rem(me + 2, n))[d - 1]
        return lax.rem(me + d, n)

    def source(d):
        return peer(d) if n == 4 else lax.rem(me + n - d, n)

    barrier = pltpu.get_barrier_semaphore()
    for d in range(1, n):
        pl.semaphore_signal(barrier, inc=1, device_id={"mp": peer(d)})
    pl.semaphore_signal(barrier, inc=1, device_id={"section": 1 - section})
    for d in range(1, shares):
        pl.semaphore_signal(barrier, inc=1, device_id={"dp": lax.rem(replica + d, shares)})
    pl.semaphore_wait(barrier, n + shares - 1)

    loads = [
        pltpu.make_async_copy(a, b, load_sem.at[k])
        for k, (a, b) in enumerate(
            [(qkv_raw_ref, w_raw), (out_w_ref, w_out), (in_w_ref, w_in), (back_w_ref, w_back)]
        )
    ]
    for load in loads:
        load.start()

    def rows_of(i, index):
        return pl.ds(pl.multiple_of(i * seq + index * rows, 16), rows)

    def image_of(i):
        return pl.ds(pl.multiple_of(i * seq, 16), seq)

    def gather_copy(kind, buf, i, d, index):
        where = rows_of(i, index)
        return pltpu.make_async_remote_copy(
            src_ref=buf.at[where],
            dst_ref=buf.at[where],
            send_sem=gather_send.at[kind, i, d - 1],
            recv_sem=gather_recv.at[kind, i, d - 1],
            device_id={"mp": peer(d)},
        )

    def gather_start(kind, buf, i):
        for d in range(1, n):
            gather_copy(kind, buf, i, d, me).start()

    def gather_wait(kind, buf, i):
        for d in range(1, n):
            gather_copy(kind, buf, i, d, me).wait_send()
            gather_copy(kind, buf, i, d, source(d)).wait_recv()

    def part_copy(kind, i, d):
        return pltpu.make_async_remote_copy(
            src_ref=sends.at[rows_of(i, peer(d))],
            dst_ref=parts.at[kind & 1, i, d - 1],
            send_sem=part_send.at[kind, i, d - 1],
            recv_sem=part_recv.at[kind, i, d - 1],
            device_id={"mp": peer(d)},
        )

    def part_start(kind, i):
        for d in range(1, n):
            part_copy(kind, i, d).start()

    def part_sum(kind, i):
        for d in range(1, n):
            part_copy(kind, i, d).wait()
        total = sends[rows_of(i, me), :].astype(F32)
        for d in range(1, n):
            total = total + parts[kind & 1, i, d - 1].astype(F32)
        return total

    def pass_copy(k, i, dst):
        return pltpu.make_async_remote_copy(
            src_ref=passed.at[i],
            dst_ref=dst,
            send_sem=pass_send.at[k, i],
            recv_sem=pass_recv.at[k, i],
            device_id={"section": 1 - section},
        )

    def row_mask(i):
        index = me * rows + lax.broadcasted_iota(jnp.int32, (rows, 1), 0)
        return index < lengths_ref[i]

    def enter(i):
        @pl.when(section == 1)
        def _():
            pass_copy(0, i, tokens.at[i]).wait_recv()

        unit, _ = normalize(tokens[i].astype(F32))
        normed[rows_of(i, me), :] = (unit * norms_ref[0:1, :] + norms_ref[1:2, :]).astype(BF)
        gather_start(0, normed, i)

    def attend(i):
        gather_wait(0, normed, i)
        here = image_of(i)
        for j in range(3):
            linear = mm(normed[here, :], w_qkv[j])
            if j == 0:
                linear = linear + time_ref[i, 0:1, :]
            if j == 2:
                linear = linear + time_ref[i, 1:2, :]
            qkv[j, here, :] = linear.astype(BF)
        key_index = lax.broadcasted_iota(jnp.int32, (1, seq), 1)
        key_mask = key_index < lengths_ref[i]
        outs = []
        for h in range(heads):
            lanes = slice(h * LANES, (h + 1) * LANES)
            scores = mm(qkv[0, here, lanes], qkv[1, here, lanes], 1, 1) * score_scale + bias[h]
            scores = jnp.where(key_mask, scores, NEG_FILL)
            top = jnp.max(scores, axis=-1, keepdims=True)
            raised = jnp.exp(scores - top)
            prob = raised / jnp.sum(raised, axis=-1, keepdims=True)
            probs[i * heads + h] = prob
            outs.append(mm(prob.astype(BF), qkv[2, here, lanes]).astype(BF))
        packed = mm(jnp.concatenate(outs, axis=1), selection(local, wide, head_size, True))
        packed = packed.astype(BF)
        mixed_heads[here, :] = packed
        sends[here, :] = mm(packed, w_out[...]).astype(BF)
        part_start(0, i)

    def middle(i):
        total = tokens[i].astype(F32) + part_sum(0, i) + out_b_ref[...]
        mixed[i] = total
        unit, _ = normalize(total)
        normed_two[rows_of(i, me), :] = (unit * norms_ref[2:3, :] + norms_ref[3:4, :]).astype(BF)
        gather_start(1, normed_two, i)

    def feed(i):
        gather_wait(1, normed_two, i)
        here = image_of(i)
        hidden = mm(normed_two[here, :], w_in[...]) + in_b_ref[...]
        square = hidden * hidden
        bent = jnp.tanh(ROOT * (hidden + CUBIC * (square * hidden)))
        half = 0.5 * (1.0 + bent)
        active[here, :] = (hidden * half).astype(BF)
        slope[here, :] = half + 0.5 * hidden * (1.0 - bent * bent) * (
            ROOT + (3.0 * CUBIC * ROOT) * square
        )
        sends[here, :] = mm(active[here, :], w_back[...]).astype(BF)
        part_start(1, i)

    def leave(i):
        out = mixed[i] + part_sum(1, i) + back_b_ref[...]

        @pl.when(section == 0)
        def _():
            passed[i] = out.astype(BF)
            pass_copy(0, i, tokens.at[i]).start()

        @pl.when(section == 1)
        def _():
            boundary_ref[i] = jnp.where(row_mask(i), out, 0.0)

    def grad_enter(i):
        @pl.when(section == 0)
        def _():
            pass_copy(1, i, grad_two.at[rows_of(i, me)]).wait_recv()
            gather_start(2, grad_two, i)

    def feed_back(i):
        gather_wait(2, grad_two, i)
        here = image_of(i)
        grad_active = mm(grad_two[here, :], w_back[...], 1, 1)
        held = (slope[here, :] * grad_active).astype(BF)
        grad_hidden[here, :] = held
        sums[6:7, :] += jnp.sum(held.astype(F32), axis=0, keepdims=True)
        sends[here, :] = mm(held, w_in[...], 1, 1).astype(BF)
        part_start(2, i)

    def middle_back(i):
        grad = part_sum(2, i)
        grad_y = grad_two[rows_of(i, me), :].astype(F32)
        grad_in, gain, offset = norm_backward(grad, mixed[i], norms_ref[2:3, :])
        total = grad_y + grad_in
        mixed[i] = total
        low = total.astype(BF)
        grad_one[rows_of(i, me), :] = low
        gather_start(3, grad_one, i)
        sums[2:3, :] += gain
        sums[3:4, :] += offset
        sums[4:5, :] += jnp.sum(low.astype(F32), axis=0, keepdims=True)
        sums[5:6, :] += jnp.sum(grad_y, axis=0, keepdims=True)

    def attend_back(i):
        gather_wait(3, grad_one, i)
        here = image_of(i)
        grad_heads = mm(grad_one[here, :], w_out[...], 1, 1).astype(BF)
        grad_heads = mm(grad_heads, selection(local, wide, head_size, False)).astype(BF)
        outs = ([], [], [])
        for h in range(heads):
            lanes = slice(h * LANES, (h + 1) * LANES)
            grad_out = grad_heads[:, lanes]
            prob = probs[i * heads + h]
            grad_prob = mm(grad_out, qkv[2, here, lanes], 1, 1)
            outs[2].append(mm(prob.astype(BF), grad_out, 0, 0).astype(BF))
            inner = jnp.sum(prob * grad_prob, axis=-1, keepdims=True)
            grad_scores = (prob * (grad_prob - inner)).astype(BF)
            score_sum[h, :, 0:seq] += grad_scores.astype(F32)
            outs[0].append((mm(grad_scores, qkv[1, here, lanes]) * score_scale).astype(BF))
            outs[1].append((mm(grad_scores, qkv[0, here, lanes], 0, 0) * score_scale).astype(BF))
        total = None
        chosen = selection(local, wide, head_size, True)
        for j in range(3):
            grad = jnp.concatenate(outs[j], axis=1)
            term = mm(grad, w_qkv[j], 1, 1)
            total = term if total is None else total + term
            grad_qkv[j, here, :] = mm(grad, chosen).astype(BF)
            if j != 1:
                columns_ref[replica, i, j // 2 : j // 2 + 1, :] = jnp.sum(
                    grad.astype(F32), axis=0, keepdims=True
                )
        sends[here, :] = total.astype(BF)
        part_start(3, i)

    def grad_leave(i):
        grad = part_sum(3, i)
        grad_in, gain, offset = norm_backward(grad, tokens[i].astype(F32), norms_ref[0:1, :])
        total = mixed[i] + grad_in

        @pl.when(section == 1)
        def _():
            passed[i] = total.astype(BF)
            pass_copy(1, i, grad_two.at[rows_of(i, me)]).start()

        @pl.when(section == 0)
        def _():
            boundary_ref[i] = total

        sums[0:1, :] += gain
        sums[1:2, :] += offset

    def each(body):
        def step(i, carry):
            body(i)
            return carry

        lax.fori_loop(0, count, step, 0)

    @pl.when(section == 0)
    def _():
        copy = pltpu.make_async_copy(images_ref, tokens, load_sem.at[4])
        copy.start()
        copy.wait()
        each(enter)

    @pl.when(section == 1)
    def _():
        copy = pltpu.make_async_copy(cotangent_ref, passed, load_sem.at[4])
        copy.start()
        copy.wait()

        def given(i):
            low = jnp.where(row_mask(i), passed[i].astype(F32), 0.0).astype(BF)
            grad_two[rows_of(i, me), :] = low
            gather_start(2, grad_two, i)

        each(given)

    sums[...] = jnp.zeros_like(sums)
    score_sum[...] = jnp.zeros_like(score_sum)
    for h in range(heads):
        spread = jnp.broadcast_to(table_ref[h : h + 1, :], (seq, 2 * seq))
        bias[h] = pltpu.roll(spread, seq + 1, 1, stride=1, stride_axis=0)[:, :seq]
    loads[0].wait()
    for j in range(3):
        low = j * local // LANES * LANES
        high = -(-(j + 1) * local // LANES) * LANES
        chosen = selection(high - low, wide, head_size, False, j * local - low)
        w_qkv[j] = mm(w_raw[:, low:high], chosen).astype(BF)
    for load in loads[1:]:
        load.wait()

    def replica_peer(d):
        return lax.rem(replica + d, shares)

    def replica_source(d):
        return lax.rem(replica + shares - d, shares)

    def share_of(index):
        return pl.ds(pl.multiple_of(index * share, 8), share)

    jobs = (
        (w_back, back_grad_ref),
        (w_in, in_grad_ref),
        (w_raw, thin_grad_ref),
    )
    paired = shares == 4
    half = replica // 2
    partner = replica + 1 - 2 * lax.rem(replica, 2)
    inner = (replica == 1) | (replica == 2)

    def across(c):
        return 2 - half if c else 3 * (1 - half)

    def own_copy(k):
        buf, dst = jobs[k]
        return pltpu.make_async_copy(
            buf.at[share_of(replica)], dst.at[0 if paired else replica], weight_own.at[k]
        )

    def weight_copy(k, index, dst, send, recv, device):
        return pltpu.make_async_remote_copy(
            src_ref=jobs[k][0].at[share_of(index)],
            dst_ref=dst,
            send_sem=weight_send.at[k, send],
            recv_sem=weight_recv.at[k, recv],
            device_id={"dp": device},
        )

    def near_copy(k):
        return weight_copy(k, partner, jobs[k][1].at[1], 0, 0, partner)

    def cross_copy(k, c):
        return weight_copy(k, across(c), crossed.at[k, c], 1 + c, 1 + c, partner)

    def forward_copy(k, c):
        return weight_copy(k, across(c), jobs[k][1].at[2], 1 + c, 3, across(c))

    def direct_copy(k, d, index):
        to = replica_peer(d)
        return weight_copy(k, to, jobs[k][1].at[index], d - 1, d - 1, to)

    def weight_job(k):
        tile = LANES if k == 2 else width // 3

        def tile_step(t, carry):
            where = pl.ds(pl.multiple_of(t * tile, LANES), tile)
            if k == 0:
                out = mm(grad_two[:, where], active[...], 0, 0)
            elif k == 1:
                out = mm(normed_two[:, where], grad_hidden[...], 0, 0)
            else:
                left = normed[:, where]
                out = [mm(left, grad_qkv[j], 0, 0) for j in range(3)]
                out.append(mm(grad_one[:, where], mixed_heads[...], 0, 0))
                out = jnp.concatenate(out, axis=1)
            jobs[k][0][where, :] = out.astype(BF)
            return carry

        lax.fori_loop(0, width // tile, tile_step, 0)
        own_copy(k).start()
        if paired:

            @pl.when(jnp.logical_not(inner))
            def _():
                cross_copy(k, 0).start()
                cross_copy(k, 1).start()

            near_copy(k).start()
        else:
            for d in range(1, shares):
                direct_copy(k, d, replica).start()

    def relay(k):
        if paired:

            @pl.when(inner)
            def _():
                buf = jobs[k][0]
                for c in range(2):
                    where = share_of(across(c))
                    cross_copy(k, c).wait_recv()
                    pair = buf[where, :].astype(F32) + crossed[k, c].astype(F32)
                    buf[where, :] = pair.astype(BF)
                    forward_copy(k, c).start()

    def weight_wait(k):
        own_copy(k).wait()
        if paired:
            near_copy(k).wait()
            for c in range(2):
                cross_copy(k, c).wait_send()
            forward_copy(k, 0).wait_recv()
        else:
            for d in range(1, shares):
                direct_copy(k, d, replica).wait_send()
                direct_copy(k, d, replica_source(d)).wait_recv()

    def later_enter(i):
        @pl.when(section == 1)
        def _():
            enter(i)

    schedule = (
        (later_enter, 0, 0, count),
        (lambda i: weight_job(0), 14, 16, 1),
        (feed_back, 11, 8, count),
        (grad_enter, 8, 21, count),
        (lambda i: weight_job(1), 18, 10, 1),
        (attend, 1, 1, count),
        (grad_leave, 19, 19, count),
        (middle, 2, 2, count),
        (lambda i: relay(1), 21, 19, 1),
        (middle_back, 14, 14, count),
        (attend_back, 17, 16, count),
        (feed, 3, 4, count),
        (lambda i: weight_job(2), 20, 21, 1),
        (leave, 4, 7, count),
        (lambda i: relay(0), 18, 21, 1),
    )
    steps = max(max(first, second) for _, first, second, _ in schedule) + count

    def tick(t, carry):
        for body, first, second, times in schedule:
            i = t - (first + section * (second - first))

            @pl.when((i >= 0) & (i < times))
            def _(body=body, i=i):
                body(i)

        return carry

    lax.fori_loop(0, steps, tick, 0)

    @pl.when(section == 0)
    def _():
        each(lambda i: pass_copy(0, i, tokens.at[i]).wait_send())

    @pl.when(section == 1)
    def _():
        each(lambda i: pass_copy(1, i, grad_two.at[rows_of(i, me)]).wait_send())

    def sum_copy(d, index):
        return pltpu.make_async_remote_copy(
            src_ref=all_sums.at[me],
            dst_ref=all_sums.at[index],
            send_sem=sum_send.at[d - 1],
            recv_sem=sum_recv.at[d - 1],
            device_id={"mp": peer(d)},
        )

    all_sums[me] = sums[...]
    for d in range(1, n):
        sum_copy(d, me).start()

    lanes = 2 * seq
    carried = [jnp.zeros((8, lanes), F32) for _ in range(heads)]
    fill = jnp.zeros((8, lanes - score_sum.shape[2]), F32)

    def shift_add(g, carried):
        where = pl.ds(pl.multiple_of(g * 8, 8), 8)
        return [
            pltpu.roll(c, 8, 1) + jnp.concatenate([score_sum[h, where, :], fill], axis=1)
            for h, c in enumerate(carried)
        ]

    relay(2)
    carried = lax.fori_loop(0, seq // 8, shift_add, carried)
    behind = 7 - lax.broadcasted_iota(jnp.int32, (8, lanes), 0)
    for h in range(heads):
        c = carried[h]
        for by in (1, 2, 4):
            c = jnp.where((behind & by) != 0, pltpu.roll(c, by, 1), c)
        table_grad_ref[replica, h : h + 1, :] = jnp.sum(c, axis=0, keepdims=True)

    for d in range(1, n):
        sum_copy(d, me).wait_send()
        sum_copy(d, source(d)).wait_recv()
    total = all_sums[0]
    for k in range(1, n):
        total = total + all_sums[k]
    kind = lax.broadcasted_iota(jnp.int32, (8, width), 0)
    small_ref[replica] = jnp.where(kind < 6, total, sums[...])

    tiny = (small_ref, table_grad_ref, columns_ref, rows_ref)

    def tiny_copy(k, d, index):
        return pltpu.make_async_remote_copy(
            src_ref=tiny[k].at[replica],
            dst_ref=tiny[k].at[index],
            send_sem=tiny_send.at[k, d - 1],
            recv_sem=tiny_recv.at[k, d - 1],
            device_id={"dp": replica_peer(d)},
        )

    rows_ref[replica] = steps_ref[...]
    for k in range(4):
        for d in range(1, shares):
            tiny_copy(k, d, replica).start()
    for k in range(3):
        weight_wait(k)
    for k in range(4):
        for d in range(1, shares):
            tiny_copy(k, d, replica).wait_send()
            tiny_copy(k, d, replica_source(d)).wait_recv()


def run_layer(sizes, args):
    n, count, rows, width, hidden_width, heads, head_size, shares = sizes
    seq = n * rows
    local_width = heads * head_size
    wide = heads * LANES
    share = width // shares
    total = count * seq
    blocks = 3 if shares == 4 else shares
    vmem = pl.BlockSpec(memory_space=pltpu.VMEM)
    anywhere = pl.BlockSpec(memory_space=pl.ANY)
    dma = pltpu.SemaphoreType.DMA
    return pl.pallas_call(
        functools.partial(layer_kernel, sizes),
        out_shape=(
            jax.ShapeDtypeStruct((count, rows, width), F32),
            jax.ShapeDtypeStruct((shares, 8, width), F32),
            jax.ShapeDtypeStruct((shares, heads, 2 * seq), F32),
            jax.ShapeDtypeStruct((shares, count, 2, wide), F32),
            jax.ShapeDtypeStruct((shares, count, width), BF),
            jax.ShapeDtypeStruct((blocks, share, 4 * local_width), BF),
            jax.ShapeDtypeStruct((blocks, share, hidden_width), BF),
            jax.ShapeDtypeStruct((blocks, share, hidden_width), BF),
        ),
        in_specs=[
            pl.BlockSpec(memory_space=pltpu.SMEM),
            anywhere,
            anywhere,
            vmem,
            vmem,
            anywhere,
            anywhere,
            vmem,
            anywhere,
            vmem,
            anywhere,
            vmem,
            vmem,
            vmem,
        ],
        out_specs=(vmem, vmem, vmem, vmem, vmem, anywhere, anywhere, anywhere),
        scratch_shapes=[
            pltpu.VMEM((width, 4 * local_width), BF),
            pltpu.VMEM((3, width, wide), BF),
            pltpu.VMEM((local_width, width), BF),
            pltpu.VMEM((width, hidden_width), BF),
            pltpu.VMEM((hidden_width, width), BF),
            pltpu.VMEM((total, width), BF),
            pltpu.VMEM((total, width), BF),
            pltpu.VMEM((total, width), BF),
            pltpu.VMEM((total, width), BF),
            pltpu.VMEM((total, hidden_width), BF),
            pltpu.VMEM((total, hidden_width), BF),
            pltpu.VMEM((3, total, wide), BF),
            pltpu.VMEM((total, local_width), BF),
            pltpu.VMEM((3, total, local_width), BF),
            pltpu.VMEM((count * heads, seq, seq), F32),
            pltpu.VMEM((total, hidden_width), F32),
            pltpu.VMEM((heads, seq, seq), F32),
            pltpu.VMEM((heads, seq, -(-seq // LANES) * LANES), F32),
            pltpu.VMEM((2, count, n - 1, rows, width), BF),
            pltpu.VMEM((total, width), BF),
            pltpu.VMEM((count, rows, width), BF),
            pltpu.VMEM((count, rows, width), BF),
            pltpu.VMEM((count, rows, width), F32),
            pltpu.VMEM((3, 2, share, hidden_width), BF),
            pltpu.VMEM((8, width), F32),
            pltpu.VMEM((n, 8, width), F32),
            dma((5,)),
            dma((4, count, n - 1)),
            dma((4, count, n - 1)),
            dma((4, count, n - 1)),
            dma((4, count, n - 1)),
            dma((2, count)),
            dma((2, count)),
            dma((3, shares)),
            dma((3, shares)),
            dma((3,)),
            dma((4, shares - 1)),
            dma((4, shares - 1)),
            dma((n - 1,)),
            dma((n - 1,)),
        ],
        compiler_params=pltpu.CompilerParams(
            collective_id=0, has_side_effects=True, vmem_limit_bytes=67043328
        ),
        name="two_pass",
    )(*args)


def local(
    images,
    cotangent,
    lengths,
    timesteps,
    time_table,
    norms,
    qkv_weight,
    time_weight,
    out_weight,
    out_bias,
    mlp_in_weight,
    mlp_in_bias,
    mlp_out_weight,
    mlp_out_bias,
    rel_bias,
):
    count, rows, width = images.shape
    local_width = qkv_weight.shape[3]
    hidden_width = mlp_in_weight.shape[2]
    heads = rel_bias.shape[1]
    head_size = local_width // heads
    shares = lax.axis_size("dp")
    share = width // shares
    sizes = (lax.axis_size("mp"), count, rows, width, hidden_width, heads, head_size, shares)
    time_rows = jnp.concatenate(
        [lax.dynamic_slice_in_dim(time_table, timesteps[i], 1, axis=0) for i in range(count)]
    )
    time_part = jnp.dot(
        time_rows, time_weight[0].reshape(width, 2 * local_width), preferred_element_type=F32
    ).reshape(count, 2, heads, head_size)
    time_part = jnp.pad(time_part, ((0, 0), (0, 0), (0, 0), (0, LANES - head_size)))
    time_part = time_part.reshape(count, 2, heads * LANES)
    table = jnp.pad(jnp.flip(rel_bias[0], axis=1), ((0, 0), (0, 1)))
    outs = run_layer(
        sizes,
        (
            lengths,
            images,
            cotangent,
            time_part,
            norms[0],
            jnp.pad(qkv_weight[0].reshape(width, 3 * local_width), ((0, 0), (0, local_width))),
            out_weight[0],
            out_bias,
            mlp_in_weight[0],
            mlp_in_bias,
            mlp_out_weight[0],
            mlp_out_bias,
            table,
            time_rows,
        ),
    )
    boundary, small, table_grad, columns, all_rows, thin_grad, in_grad, back_grad = outs
    columns = columns.reshape(shares * count, 2, heads, LANES)[..., :head_size]
    columns = columns.reshape(shares * count, 2 * local_width)
    all_rows = lax.dynamic_slice_in_dim(
        all_rows.reshape(shares * count, width), lax.axis_index("dp") * share, share, axis=1
    )
    time_grad = lax.dot_general(
        all_rows.astype(F32),
        columns,
        (((0,), (0,)), ((), ())),
        precision=lax.Precision.HIGHEST,
        preferred_element_type=F32,
    ).reshape(share, 2, local_width)

    def added(value):
        return jnp.sum(value.astype(F32), axis=0)

    small = added(small)
    thin_grad = added(thin_grad)
    table_grad = jnp.flip(added(table_grad)[:, : rel_bias.shape[2]], axis=1)
    return (
        boundary[None],
        small[None, :4],
        thin_grad[:, : 3 * local_width].reshape(share, 3, local_width)[None],
        time_grad[None],
        thin_grad[:, 3 * local_width :].T[None],
        small[4][None],
        added(in_grad)[None],
        small[6][None],
        added(back_grad).T[None],
        small[5][None],
        table_grad[None],
    )


def solution(mesh):
    in_specs = (
        P("dp", "mp", None),
        P("dp", "mp", None),
        P("dp"),
        P("dp"),
        P(),
        P("section", None, None),
        P("section", None, None, "mp"),
        P("section", None, None, "mp"),
        P("section", "mp", None),
        P("section", None),
        P("section", None, "mp"),
        P("section", "mp"),
        P("section", "mp", None),
        P("section", None),
        P("section", "mp", None),
    )
    out_specs = (
        P("section", "dp", "mp", None),
        P("section", None, None),
        P("section", "dp", None, "mp"),
        P("section", "dp", None, "mp"),
        P("section", "mp", "dp"),
        P("section", None),
        P("section", "dp", "mp"),
        P("section", "mp"),
        P("section", "mp", "dp"),
        P("section", None),
        P("section", "mp", None),
    )
    return jax.shard_map(local, mesh=mesh, in_specs=in_specs, out_specs=out_specs, check_vma=False)
```

```python
import functools
import math

import jax
import jax.numpy as jnp
from jax import lax
from jax.experimental import pallas as pl
from jax.experimental.pallas import tpu as pltpu
from jax.sharding import PartitionSpec as P

EPSILON = 1e-06
NEG_FILL = -1000000000.0
LANES = 128
BF = jnp.bfloat16
F32 = jnp.float32
ROOT = math.sqrt(2.0 / math.pi)
CUBIC = 0.044715


def mm(left, right, left_dim=1, right_dim=0):
    return lax.dot_general(
        left, right, (((left_dim,), (right_dim,)), ((), ())), preferred_element_type=F32
    )


def selection(rows, cols, head_size, flip):
    shape = (cols, rows) if flip else (rows, cols)
    row = lax.broadcasted_iota(jnp.int32, shape, 1 if flip else 0)
    col = lax.broadcasted_iota(jnp.int32, shape, 0 if flip else 1)
    within = col & (LANES - 1)
    hit = (within < head_size) & (row == (col // LANES) * head_size + within)
    return jnp.where(hit, 1.0, 0.0).astype(BF)


def normalize(values):
    centred = values - jnp.mean(values, axis=-1, keepdims=True)
    spread = jnp.mean(centred * centred, axis=-1, keepdims=True)
    scale = lax.rsqrt(spread + EPSILON)
    return centred * scale, scale


def norm_backward(grad, values, gain):
    unit, scale = normalize(values)
    inner = grad * gain
    mean_one = jnp.mean(inner, axis=-1, keepdims=True)
    mean_two = jnp.mean(inner * unit, axis=-1, keepdims=True)
    grad_in = scale * (inner - mean_one - unit * mean_two)
    gain_grad = jnp.sum(grad * unit, axis=0, keepdims=True)
    offset_grad = jnp.sum(grad, axis=0, keepdims=True)
    return grad_in, gain_grad, offset_grad


def layer_kernel(
    sizes,
    lengths_ref,
    images_ref,
    cotangent_ref,
    time_ref,
    norms_ref,
    qkv_raw_ref,
    out_w_ref,
    out_b_ref,
    in_w_ref,
    in_b_ref,
    back_w_ref,
    back_b_ref,
    table_ref,
    steps_ref,
    boundary_ref,
    small_ref,
    table_grad_ref,
    columns_ref,
    rows_ref,
    thin_grad_ref,
    in_grad_ref,
    back_grad_ref,
    w_raw,
    w_qkv,
    w_out,
    w_in,
    w_back,
    normed,
    normed_two,
    grad_two,
    grad_one,
    active,
    grad_hidden,
    qkv,
    mixed_heads,
    grad_qkv,
    probs,
    slope,
    bias,
    score_sum,
    parts,
    sends,
    tokens,
    passed,
    mixed,
    crossed,
    sums,
    all_sums,
    load_sem,
    gather_send,
    gather_recv,
    part_send,
    part_recv,
    pass_send,
    pass_recv,
    weight_send,
    weight_recv,
    weight_own,
    tiny_send,
    tiny_recv,
    sum_send,
    sum_recv,
):
    n, count, rows, width, hidden_width, heads, head_size, shares = sizes
    seq = n * rows
    local = heads * head_size
    wide = heads * LANES
    share = width // shares
    score_scale = 1.0 / math.sqrt(head_size)
    me = lax.axis_index("mp")
    section = lax.axis_index("section")
    replica = lax.axis_index("dp")
    own = pl.multiple_of(me * rows, 16)

    def peer(d):
        if n == 4:
            return (n - 1 - me, me + 1 - 2 * lax.rem(me, 2), lax.rem(me + 2, n))[d - 1]
        return lax.rem(me + d, n)

    def source(d):
        return peer(d) if n == 4 else lax.rem(me + n - d, n)

    barrier = pltpu.get_barrier_semaphore()
    for d in range(1, n):
        pl.semaphore_signal(barrier, inc=1, device_id={"mp": peer(d)})
    pl.semaphore_signal(barrier, inc=1, device_id={"section": 1 - section})
    for d in range(1, shares):
        pl.semaphore_signal(barrier, inc=1, device_id={"dp": lax.rem(replica + d, shares)})
    pl.semaphore_wait(barrier, n + shares - 1)

    loads = [
        pltpu.make_async_copy(a, b, load_sem.at[k])
        for k, (a, b) in enumerate(
            [(qkv_raw_ref, w_raw.at[0 : 3 * local]), (out_w_ref, w_out), (in_w_ref, w_in), (back_w_ref, w_back)]
        )
    ]
    for load in loads:
        load.start()

    def rows_of(i, index):
        return pl.ds(pl.multiple_of(i * seq + index * rows, 16), rows)

    def image_of(i):
        return pl.ds(pl.multiple_of(i * seq, 16), seq)

    def gather_copy(kind, buf, i, d, index):
        where = rows_of(i, index)
        return pltpu.make_async_remote_copy(
            src_ref=buf.at[where],
            dst_ref=buf.at[where],
            send_sem=gather_send.at[kind, i, d - 1],
            recv_sem=gather_recv.at[kind, i, d - 1],
            device_id={"mp": peer(d)},
        )

    def gather_start(kind, buf, i):
        for d in range(1, n):
            gather_copy(kind, buf, i, d, me).start()

    def gather_wait(kind, buf, i):
        for d in range(1, n):
            gather_copy(kind, buf, i, d, me).wait_send()
            gather_copy(kind, buf, i, d, source(d)).wait_recv()

    def part_copy(kind, i, d):
        return pltpu.make_async_remote_copy(
            src_ref=sends.at[rows_of(i, peer(d))],
            dst_ref=parts.at[kind & 1, i, d - 1],
            send_sem=part_send.at[kind, i, d - 1],
            recv_sem=part_recv.at[kind, i, d - 1],
            device_id={"mp": peer(d)},
        )

    def part_start(kind, i):
        for d in range(1, n):
            part_copy(kind, i, d).start()

    def part_sum(kind, i):
        for d in range(1, n):
            part_copy(kind, i, d).wait()
        total = sends[rows_of(i, me), :].astype(F32)
        for d in range(1, n):
            total = total + parts[kind & 1, i, d - 1].astype(F32)
        return total

    def pass_copy(k, i, dst):
        return pltpu.make_async_remote_copy(
            src_ref=passed.at[i],
            dst_ref=dst,
            send_sem=pass_send.at[k, i],
            recv_sem=pass_recv.at[k, i],
            device_id={"section": 1 - section},
        )

    def row_mask(i):
        index = me * rows + lax.broadcasted_iota(jnp.int32, (rows, 1), 0)
        return index < lengths_ref[i]

    def enter(i):
        @pl.when(section == 1)
        def _():
            pass_copy(0, i, tokens.at[i]).wait_recv()

        unit, _ = normalize(tokens[i].astype(F32))
        normed[rows_of(i, me), :] = (unit * norms_ref[0:1, :] + norms_ref[1:2, :]).astype(BF)
        gather_start(0, normed, i)

    def attend(i):
        gather_wait(0, normed, i)
        here = image_of(i)
        for j in range(3):
            linear = mm(normed[here, :], w_qkv[j], 1, 1)
            if j == 0:
                linear = linear + time_ref[i, 0:1, :]
            if j == 2:
                linear = linear + time_ref[i, 1:2, :]
            qkv[j, here, :] = linear.astype(BF)
        key_index = lax.broadcasted_iota(jnp.int32, (1, seq), 1)
        key_mask = key_index < lengths_ref[i]
        outs = []
        for h in range(heads):
            lanes = slice(h * LANES, (h + 1) * LANES)
            scores = mm(qkv[0, here, lanes], qkv[1, here, lanes], 1, 1) * score_scale + bias[h]
            scores = jnp.where(key_mask, scores, NEG_FILL)
            top = jnp.max(scores, axis=-1, keepdims=True)
            raised = jnp.exp(scores - top)
            prob = raised / jnp.sum(raised, axis=-1, keepdims=True)
            probs[i * heads + h] = prob
            outs.append(mm(prob.astype(BF), qkv[2, here, lanes]).astype(BF))
        packed = mm(jnp.concatenate(outs, axis=1), selection(local, wide, head_size, True))
        packed = packed.astype(BF)
        mixed_heads[here, :] = packed
        sends[here, :] = mm(packed, w_out[...]).astype(BF)
        part_start(0, i)

    def middle(i):
        total = tokens[i].astype(F32) + part_sum(0, i) + out_b_ref[...]
        mixed[i] = total
        unit, _ = normalize(total)
        normed_two[rows_of(i, me), :] = (unit * norms_ref[2:3, :] + norms_ref[3:4, :]).astype(BF)
        gather_start(1, normed_two, i)

    def feed(i):
        gather_wait(1, normed_two, i)
        here = image_of(i)
        hidden = mm(normed_two[here, :], w_in[...]) + in_b_ref[...]
        square = hidden * hidden
        bent = jnp.tanh(ROOT * (hidden + CUBIC * (square * hidden)))
        half = 0.5 * (1.0 + bent)
        active[here, :] = (hidden * half).astype(BF)
        slope[here, :] = half + 0.5 * hidden * (1.0 - bent * bent) * (
            ROOT + (3.0 * CUBIC * ROOT) * square
        )
        sends[here, :] = mm(active[here, :], w_back[...]).astype(BF)
        part_start(1, i)

    def leave(i):
        out = mixed[i] + part_sum(1, i) + back_b_ref[...]

        @pl.when(section == 0)
        def _():
            passed[i] = out.astype(BF)
            pass_copy(0, i, tokens.at[i]).start()

        @pl.when(section == 1)
        def _():
            boundary_ref[i] = jnp.where(row_mask(i), out, 0.0)

    def grad_enter(i):
        @pl.when(section == 0)
        def _():
            pass_copy(1, i, grad_two.at[rows_of(i, me)]).wait_recv()
            gather_start(2, grad_two, i)

    def feed_back(i):
        gather_wait(2, grad_two, i)
        here = image_of(i)
        grad_active = mm(grad_two[here, :], w_back[...], 1, 1)
        held = (slope[here, :] * grad_active).astype(BF)
        grad_hidden[here, :] = held
        sums[6:7, :] += jnp.sum(held.astype(F32), axis=0, keepdims=True)
        sends[here, :] = mm(held, w_in[...], 1, 1).astype(BF)
        part_start(2, i)

    def middle_back(i):
        grad = part_sum(2, i)
        grad_y = grad_two[rows_of(i, me), :].astype(F32)
        grad_in, gain, offset = norm_backward(grad, mixed[i], norms_ref[2:3, :])
        total = grad_y + grad_in
        mixed[i] = total
        low = total.astype(BF)
        grad_one[rows_of(i, me), :] = low
        gather_start(3, grad_one, i)
        sums[2:3, :] += gain
        sums[3:4, :] += offset
        sums[4:5, :] += jnp.sum(low.astype(F32), axis=0, keepdims=True)
        sums[5:6, :] += jnp.sum(grad_y, axis=0, keepdims=True)

    def attend_back(i):
        gather_wait(3, grad_one, i)
        here = image_of(i)
        grad_heads = mm(grad_one[here, :], w_out[...], 1, 1).astype(BF)
        grad_heads = mm(grad_heads, selection(local, wide, head_size, False)).astype(BF)
        outs = ([], [], [])
        for h in range(heads):
            lanes = slice(h * LANES, (h + 1) * LANES)
            grad_out = grad_heads[:, lanes]
            prob = probs[i * heads + h]
            grad_prob = mm(grad_out, qkv[2, here, lanes], 1, 1)
            outs[2].append(mm(prob.astype(BF), grad_out, 0, 0).astype(BF))
            inner = jnp.sum(prob * grad_prob, axis=-1, keepdims=True)
            grad_scores = (prob * (grad_prob - inner)).astype(BF)
            score_sum[h, :, 0:seq] += grad_scores.astype(F32)
            outs[0].append((mm(grad_scores, qkv[1, here, lanes]) * score_scale).astype(BF))
            outs[1].append((mm(grad_scores, qkv[0, here, lanes], 0, 0) * score_scale).astype(BF))
        total = None
        chosen = selection(local, wide, head_size, True)
        for j in range(3):
            grad = jnp.concatenate(outs[j], axis=1)
            term = mm(grad, w_qkv[j])
            total = term if total is None else total + term
            grad_qkv[j, here, :] = mm(grad, chosen).astype(BF)
            if j != 1:
                columns_ref[replica, i, j // 2 : j // 2 + 1, :] = jnp.sum(
                    grad.astype(F32), axis=0, keepdims=True
                )
        sends[here, :] = total.astype(BF)
        part_start(3, i)

    def grad_leave(i):
        grad = part_sum(3, i)
        grad_in, gain, offset = norm_backward(grad, tokens[i].astype(F32), norms_ref[0:1, :])
        total = mixed[i] + grad_in

        @pl.when(section == 1)
        def _():
            passed[i] = total.astype(BF)
            pass_copy(1, i, grad_two.at[rows_of(i, me)]).start()

        @pl.when(section == 0)
        def _():
            boundary_ref[i] = total

        sums[0:1, :] += gain
        sums[1:2, :] += offset

    def each(body):
        def step(i, carry):
            body(i)
            return carry

        lax.fori_loop(0, count, step, 0)

    @pl.when(section == 0)
    def _():
        copy = pltpu.make_async_copy(images_ref, tokens, load_sem.at[4])
        copy.start()
        copy.wait()
        each(enter)

    @pl.when(section == 1)
    def _():
        copy = pltpu.make_async_copy(cotangent_ref, passed, load_sem.at[4])
        copy.start()
        copy.wait()

        def given(i):
            low = jnp.where(row_mask(i), passed[i].astype(F32), 0.0).astype(BF)
            grad_two[rows_of(i, me), :] = low
            gather_start(2, grad_two, i)

        each(given)

    sums[...] = jnp.zeros_like(sums)
    score_sum[...] = jnp.zeros_like(score_sum)
    for h in range(heads):
        spread = jnp.broadcast_to(table_ref[h : h + 1, :], (seq, 2 * seq))
        bias[h] = pltpu.roll(spread, seq + 1, 1, stride=1, stride_axis=0)[:, :seq]
    loads[0].wait()
    chosen = selection(local, wide, head_size, True)
    for j in range(3):
        w_qkv[j] = mm(chosen, w_raw[j * local : (j + 1) * local, :]).astype(BF)
    for load in loads[1:]:
        load.wait()

    def replica_peer(d):
        return lax.rem(replica + d, shares)

    def replica_source(d):
        return lax.rem(replica + shares - d, shares)

    def share_of(index):
        return pl.ds(pl.multiple_of(index * share, 8), share)

    jobs = (
        (w_back, back_grad_ref),
        (w_in, in_grad_ref),
        (w_raw, thin_grad_ref),
    )
    tile = width // 3
    paired = shares == 4
    half = replica // 2
    partner = replica + 1 - 2 * lax.rem(replica, 2)
    inner = (replica == 1) | (replica == 2)

    def across(c):
        return 2 - half if c else 3 * (1 - half)

    def own_copy(k):
        buf, dst = jobs[k]
        return pltpu.make_async_copy(
            buf.at[share_of(replica)], dst.at[0 if paired else replica], weight_own.at[k]
        )

    def weight_copy(k, index, dst, send, recv, device):
        return pltpu.make_async_remote_copy(
            src_ref=jobs[k][0].at[share_of(index)],
            dst_ref=dst,
            send_sem=weight_send.at[k, send],
            recv_sem=weight_recv.at[k, recv],
            device_id={"dp": device},
        )

    def near_copy(k):
        return weight_copy(k, partner, jobs[k][1].at[1], 0, 0, partner)

    def cross_copy(k, c):
        return weight_copy(k, across(c), crossed.at[k, c], 1 + c, 1 + c, partner)

    def forward_copy(k, c):
        return weight_copy(k, across(c), jobs[k][1].at[2], 1 + c, 3, across(c))

    def direct_copy(k, d, index):
        to = replica_peer(d)
        return weight_copy(k, to, jobs[k][1].at[index], d - 1, d - 1, to)

    def weight_job(k):
        def tile_step(t, carry):
            place = 2 - t + half * (2 * t - 2) if paired else t
            where = pl.ds(pl.multiple_of(place * tile, LANES), tile)
            if k == 0:
                out = mm(grad_two[:, where], active[...], 0, 0)
            elif k == 1:
                out = mm(normed_two[:, where], grad_hidden[...], 0, 0)
            else:
                left = normed[:, where]
                out = [mm(left, grad_qkv[j], 0, 0) for j in range(3)]
                out.append(mm(grad_one[:, where], mixed_heads[...], 0, 0))
                out = jnp.concatenate(out, axis=1)
            jobs[k][0][where, :] = out.astype(BF)
            if paired:
                for c in range(2):

                    @pl.when(jnp.logical_not(inner) & (t == c))
                    def _(c=c):
                        cross_copy(k, c).start()

            return carry

        lax.fori_loop(0, 3, tile_step, 0)
        own_copy(k).start()
        if paired:
            near_copy(k).start()
        else:
            for d in range(1, shares):
                direct_copy(k, d, replica).start()

    def relay(k):
        if paired:

            @pl.when(inner)
            def _():
                buf = jobs[k][0]
                for c in range(2):
                    where = share_of(across(c))
                    cross_copy(k, c).wait_recv()
                    pair = buf[where, :].astype(F32) + crossed[k, c].astype(F32)
                    buf[where, :] = pair.astype(BF)
                    forward_copy(k, c).start()

    def weight_wait(k):
        own_copy(k).wait()
        if paired:
            near_copy(k).wait()
            for c in range(2):
                cross_copy(k, c).wait_send()
            forward_copy(k, 0).wait_recv()
        else:
            for d in range(1, shares):
                direct_copy(k, d, replica).wait_send()
                direct_copy(k, d, replica_source(d)).wait_recv()

    def later_enter(i):
        @pl.when(section == 1)
        def _():
            enter(i)

    schedule = (
        (later_enter, 0, 0, count),
        (lambda i: weight_job(0), 14, 16, 1),
        (feed_back, 11, 8, count),
        (grad_enter, 8, 21, count),
        (lambda i: weight_job(1), 18, 10, 1),
        (attend, 1, 1, count),
        (grad_leave, 19, 19, count),
        (middle, 2, 2, count),
        (lambda i: relay(1), 21, 19, 1),
        (middle_back, 14, 14, count),
        (attend_back, 17, 16, count),
        (feed, 3, 4, count),
        (lambda i: weight_job(2), 20, 21, 1),
        (leave, 4, 7, count),
        (lambda i: relay(0), 18, 21, 1),
    )
    steps = max(max(first, second) for _, first, second, _ in schedule) + count

    def tick(t, carry):
        for body, first, second, times in schedule:
            i = t - (first + section * (second - first))

            @pl.when((i >= 0) & (i < times))
            def _(body=body, i=i):
                body(i)

        return carry

    lax.fori_loop(0, steps, tick, 0)

    @pl.when(section == 0)
    def _():
        each(lambda i: pass_copy(0, i, tokens.at[i]).wait_send())

    @pl.when(section == 1)
    def _():
        each(lambda i: pass_copy(1, i, grad_two.at[rows_of(i, me)]).wait_send())

    def sum_copy(d, index):
        return pltpu.make_async_remote_copy(
            src_ref=all_sums.at[me],
            dst_ref=all_sums.at[index],
            send_sem=sum_send.at[d - 1],
            recv_sem=sum_recv.at[d - 1],
            device_id={"mp": peer(d)},
        )

    all_sums[me] = sums[...]
    for d in range(1, n):
        sum_copy(d, me).start()

    lanes = 2 * seq
    carried = [jnp.zeros((8, lanes), F32) for _ in range(heads)]
    fill = jnp.zeros((8, lanes - score_sum.shape[2]), F32)

    def shift_add(g, carried):
        where = pl.ds(pl.multiple_of(g * 8, 8), 8)
        return [
            pltpu.roll(c, 8, 1) + jnp.concatenate([score_sum[h, where, :], fill], axis=1)
            for h, c in enumerate(carried)
        ]

    relay(2)
    carried = lax.fori_loop(0, seq // 8, shift_add, carried)
    behind = 7 - lax.broadcasted_iota(jnp.int32, (8, lanes), 0)
    for h in range(heads):
        c = carried[h]
        for by in (1, 2, 4):
            c = jnp.where((behind & by) != 0, pltpu.roll(c, by, 1), c)
        table_grad_ref[replica, h : h + 1, :] = jnp.sum(c, axis=0, keepdims=True)

    for d in range(1, n):
        sum_copy(d, me).wait_send()
        sum_copy(d, source(d)).wait_recv()
    total = all_sums[0]
    for k in range(1, n):
        total = total + all_sums[k]
    kind = lax.broadcasted_iota(jnp.int32, (8, width), 0)
    small_ref[replica] = jnp.where(kind < 6, total, sums[...])

    tiny = (small_ref, table_grad_ref, columns_ref, rows_ref)

    def tiny_copy(k, d, index):
        return pltpu.make_async_remote_copy(
            src_ref=tiny[k].at[replica],
            dst_ref=tiny[k].at[index],
            send_sem=tiny_send.at[k, d - 1],
            recv_sem=tiny_recv.at[k, d - 1],
            device_id={"dp": replica_peer(d)},
        )

    rows_ref[replica] = steps_ref[...]
    for k in range(4):
        for d in range(1, shares):
            tiny_copy(k, d, replica).start()
    for k in range(3):
        weight_wait(k)
    for k in range(4):
        for d in range(1, shares):
            tiny_copy(k, d, replica).wait_send()
            tiny_copy(k, d, replica_source(d)).wait_recv()


def run_layer(sizes, args):
    n, count, rows, width, hidden_width, heads, head_size, shares = sizes
    seq = n * rows
    local_width = heads * head_size
    wide = heads * LANES
    share = width // shares
    total = count * seq
    blocks = 3 if shares == 4 else shares
    vmem = pl.BlockSpec(memory_space=pltpu.VMEM)
    anywhere = pl.BlockSpec(memory_space=pl.ANY)
    dma = pltpu.SemaphoreType.DMA
    return pl.pallas_call(
        functools.partial(layer_kernel, sizes),
        out_shape=(
            jax.ShapeDtypeStruct((count, rows, width), F32),
            jax.ShapeDtypeStruct((shares, 8, width), F32),
            jax.ShapeDtypeStruct((shares, heads, 2 * seq), F32),
            jax.ShapeDtypeStruct((shares, count, 2, wide), F32),
            jax.ShapeDtypeStruct((shares, count, width), BF),
            jax.ShapeDtypeStruct((blocks, share, 4 * local_width), BF),
            jax.ShapeDtypeStruct((blocks, share, hidden_width), BF),
            jax.ShapeDtypeStruct((blocks, share, hidden_width), BF),
        ),
        in_specs=[
            pl.BlockSpec(memory_space=pltpu.SMEM),
            anywhere,
            anywhere,
            vmem,
            vmem,
            anywhere,
            anywhere,
            vmem,
            anywhere,
            vmem,
            anywhere,
            vmem,
            vmem,
            vmem,
        ],
        out_specs=(vmem, vmem, vmem, vmem, vmem, anywhere, anywhere, anywhere),
        scratch_shapes=[
            pltpu.VMEM((width, 4 * local_width), BF),
            pltpu.VMEM((3, wide, width), BF),
            pltpu.VMEM((local_width, width), BF),
            pltpu.VMEM((width, hidden_width), BF),
            pltpu.VMEM((hidden_width, width), BF),
            pltpu.VMEM((total, width), BF),
            pltpu.VMEM((total, width), BF),
            pltpu.VMEM((total, width), BF),
            pltpu.VMEM((total, width), BF),
            pltpu.VMEM((total, hidden_width), BF),
            pltpu.VMEM((total, hidden_width), BF),
            pltpu.VMEM((3, total, wide), BF),
            pltpu.VMEM((total, local_width), BF),
            pltpu.VMEM((3, total, local_width), BF),
            pltpu.VMEM((count * heads, seq, seq), F32),
            pltpu.VMEM((total, hidden_width), F32),
            pltpu.VMEM((heads, seq, seq), F32),
            pltpu.VMEM((heads, seq, -(-seq // LANES) * LANES), F32),
            pltpu.VMEM((2, count, n - 1, rows, width), BF),
            pltpu.VMEM((total, width), BF),
            pltpu.VMEM((count, rows, width), BF),
            pltpu.VMEM((count, rows, width), BF),
            pltpu.VMEM((count, rows, width), F32),
            pltpu.VMEM((3, 2, share, hidden_width), BF),
            pltpu.VMEM((8, width), F32),
            pltpu.VMEM((n, 8, width), F32),
            dma((5,)),
            dma((4, count, n - 1)),
            dma((4, count, n - 1)),
            dma((4, count, n - 1)),
            dma((4, count, n - 1)),
            dma((2, count)),
            dma((2, count)),
            dma((3, shares)),
            dma((3, shares)),
            dma((3,)),
            dma((4, shares - 1)),
            dma((4, shares - 1)),
            dma((n - 1,)),
            dma((n - 1,)),
        ],
        compiler_params=pltpu.CompilerParams(
            collective_id=0, has_side_effects=True, vmem_limit_bytes=67043328
        ),
        name="two_pass",
    )(*args)


def local(
    images,
    cotangent,
    lengths,
    timesteps,
    time_table,
    norms,
    qkv_weight,
    time_weight,
    out_weight,
    out_bias,
    mlp_in_weight,
    mlp_in_bias,
    mlp_out_weight,
    mlp_out_bias,
    rel_bias,
):
    count, rows, width = images.shape
    local_width = qkv_weight.shape[3]
    hidden_width = mlp_in_weight.shape[2]
    heads = rel_bias.shape[1]
    head_size = local_width // heads
    shares = lax.axis_size("dp")
    share = width // shares
    sizes = (lax.axis_size("mp"), count, rows, width, hidden_width, heads, head_size, shares)
    chosen = jax.nn.one_hot(timesteps, time_table.shape[0], dtype=BF)
    time_rows = jnp.dot(chosen, time_table, preferred_element_type=F32).astype(BF)
    time_part = jnp.dot(
        time_rows, time_weight[0].reshape(width, 2 * local_width), preferred_element_type=F32
    ).reshape(count, 2, heads, head_size)
    time_part = jnp.pad(time_part, ((0, 0), (0, 0), (0, 0), (0, LANES - head_size)))
    time_part = time_part.reshape(count, 2, heads * LANES)
    table = jnp.pad(jnp.flip(rel_bias[0], axis=1), ((0, 0), (0, 1)))
    outs = run_layer(
        sizes,
        (
            lengths,
            images,
            cotangent,
            time_part,
            norms[0],
            jnp.transpose(qkv_weight[0], (1, 2, 0)).reshape(3 * local_width, width),
            out_weight[0],
            out_bias,
            mlp_in_weight[0],
            mlp_in_bias,
            mlp_out_weight[0],
            mlp_out_bias,
            table,
            time_rows,
        ),
    )
    boundary, small, table_grad, columns, all_rows, thin_grad, in_grad, back_grad = outs
    columns = columns.reshape(shares * count, 2, heads, LANES)[..., :head_size]
    columns = columns.reshape(shares * count, 2 * local_width)
    all_rows = lax.dynamic_slice_in_dim(
        all_rows.reshape(shares * count, width), lax.axis_index("dp") * share, share, axis=1
    )
    time_grad = lax.dot_general(
        all_rows.astype(F32),
        columns,
        (((0,), (0,)), ((), ())),
        precision=lax.Precision.HIGHEST,
        preferred_element_type=F32,
    ).reshape(share, 2, local_width)

    def added(value):
        return jnp.sum(value.astype(F32), axis=0)

    small = added(small)
    thin_grad = added(thin_grad)
    table_grad = jnp.flip(added(table_grad)[:, : rel_bias.shape[2]], axis=1)
    return (
        boundary[None],
        small[None, :4],
        thin_grad[:, : 3 * local_width].reshape(share, 3, local_width)[None],
        time_grad[None],
        thin_grad[:, 3 * local_width :].T[None],
        small[4][None],
        added(in_grad)[None],
        small[6][None],
        added(back_grad).T[None],
        small[5][None],
        table_grad[None],
    )


def solution(mesh):
    in_specs = (
        P("dp", "mp", None),
        P("dp", "mp", None),
        P("dp"),
        P("dp"),
        P(),
        P("section", None, None),
        P("section", None, None, "mp"),
        P("section", None, None, "mp"),
        P("section", "mp", None),
        P("section", None),
        P("section", None, "mp"),
        P("section", "mp"),
        P("section", "mp", None),
        P("section", None),
        P("section", "mp", None),
    )
    out_specs = (
        P("section", "dp", "mp", None),
        P("section", None, None),
        P("section", "dp", None, "mp"),
        P("section", "dp", None, "mp"),
        P("section", "mp", "dp"),
        P("section", None),
        P("section", "dp", "mp"),
        P("section", "mp"),
        P("section", "mp", "dp"),
        P("section", None),
        P("section", "mp", None),
    )
    return jax.shard_map(local, mesh=mesh, in_specs=in_specs, out_specs=out_specs, check_vma=False)
```

```python
import functools
import math

import jax
import jax.numpy as jnp
from jax import lax
from jax.experimental import pallas as pl
from jax.experimental.pallas import tpu as pltpu
from jax.sharding import PartitionSpec as P

EPSILON = 1e-06
NEG_FILL = -1000000000.0
LANES = 128
BF = jnp.bfloat16
F32 = jnp.float32
ROOT = math.sqrt(2.0 / math.pi)
CUBIC = 0.044715


def mm(left, right, left_dim=1, right_dim=0):
    return lax.dot_general(
        left, right, (((left_dim,), (right_dim,)), ((), ())), preferred_element_type=F32
    )


def selection(rows, cols, head_size, flip):
    shape = (cols, rows) if flip else (rows, cols)
    row = lax.broadcasted_iota(jnp.int32, shape, 1 if flip else 0)
    col = lax.broadcasted_iota(jnp.int32, shape, 0 if flip else 1)
    within = col & (LANES - 1)
    hit = (within < head_size) & (row == (col // LANES) * head_size + within)
    return jnp.where(hit, 1.0, 0.0).astype(BF)


def normalize(values):
    centred = values - jnp.mean(values, axis=-1, keepdims=True)
    spread = jnp.mean(centred * centred, axis=-1, keepdims=True)
    scale = lax.rsqrt(spread + EPSILON)
    return centred * scale, scale


def norm_backward(grad, values, gain):
    unit, scale = normalize(values)
    inner = grad * gain
    mean_one = jnp.mean(inner, axis=-1, keepdims=True)
    mean_two = jnp.mean(inner * unit, axis=-1, keepdims=True)
    grad_in = scale * (inner - mean_one - unit * mean_two)
    gain_grad = jnp.sum(grad * unit, axis=0, keepdims=True)
    offset_grad = jnp.sum(grad, axis=0, keepdims=True)
    return grad_in, gain_grad, offset_grad


def layer_kernel(
    sizes,
    lengths_ref,
    images_ref,
    cotangent_ref,
    time_ref,
    norms_ref,
    qkv_raw_ref,
    out_w_ref,
    out_b_ref,
    in_w_ref,
    in_b_ref,
    back_w_ref,
    back_b_ref,
    table_ref,
    steps_ref,
    boundary_ref,
    small_ref,
    table_grad_ref,
    columns_ref,
    rows_ref,
    thin_grad_ref,
    in_grad_ref,
    back_grad_ref,
    w_raw,
    w_qkv,
    w_out,
    w_in,
    w_back,
    normed,
    normed_two,
    grad_two,
    grad_one,
    active,
    grad_hidden,
    qkv,
    mixed_heads,
    grad_qkv,
    probs,
    slope,
    bias,
    score_sum,
    parts,
    sends,
    tokens,
    passed,
    mixed,
    crossed,
    sums,
    all_sums,
    load_sem,
    gather_send,
    gather_recv,
    part_send,
    part_recv,
    pass_send,
    pass_recv,
    weight_send,
    weight_recv,
    weight_own,
    tiny_send,
    tiny_recv,
    sum_send,
    sum_recv,
):
    n, count, rows, width, hidden_width, heads, head_size, shares = sizes
    seq = n * rows
    local = heads * head_size
    wide = heads * LANES
    share = width // shares
    score_scale = 1.0 / math.sqrt(head_size)
    me = lax.axis_index("mp")
    section = lax.axis_index("section")
    replica = lax.axis_index("dp")
    own = pl.multiple_of(me * rows, 16)

    def peer(d):
        if n == 4:
            return (n - 1 - me, me + 1 - 2 * lax.rem(me, 2), lax.rem(me + 2, n))[d - 1]
        return lax.rem(me + d, n)

    def source(d):
        return peer(d) if n == 4 else lax.rem(me + n - d, n)

    barrier = pltpu.get_barrier_semaphore()
    for d in range(1, n):
        pl.semaphore_signal(barrier, inc=1, device_id={"mp": peer(d)})
    pl.semaphore_signal(barrier, inc=1, device_id={"section": 1 - section})
    for d in range(1, shares):
        pl.semaphore_signal(barrier, inc=1, device_id={"dp": lax.rem(replica + d, shares)})
    pl.semaphore_wait(barrier, n + shares - 1)

    loads = [
        pltpu.make_async_copy(a, b, load_sem.at[k])
        for k, (a, b) in enumerate(
            [(qkv_raw_ref, w_raw.at[0 : 3 * local]), (out_w_ref, w_out), (in_w_ref, w_in), (back_w_ref, w_back)]
        )
    ]
    for load in loads:
        load.start()

    def rows_of(i, index):
        return pl.ds(pl.multiple_of(i * seq + index * rows, 16), rows)

    def image_of(i):
        return pl.ds(pl.multiple_of(i * seq, 16), seq)

    def gather_copy(kind, buf, i, d, index):
        where = rows_of(i, index)
        return pltpu.make_async_remote_copy(
            src_ref=buf.at[where],
            dst_ref=buf.at[where],
            send_sem=gather_send.at[kind, i, d - 1],
            recv_sem=gather_recv.at[kind, i, d - 1],
            device_id={"mp": peer(d)},
        )

    def gather_start(kind, buf, i):
        for d in range(1, n):
            gather_copy(kind, buf, i, d, me).start()

    def gather_wait(kind, buf, i):
        for d in range(1, n):
            gather_copy(kind, buf, i, d, me).wait_send()
            gather_copy(kind, buf, i, d, source(d)).wait_recv()

    def part_copy(kind, i, d):
        return pltpu.make_async_remote_copy(
            src_ref=sends.at[rows_of(i, peer(d))],
            dst_ref=parts.at[kind & 1, i, d - 1],
            send_sem=part_send.at[kind, i, d - 1],
            recv_sem=part_recv.at[kind, i, d - 1],
            device_id={"mp": peer(d)},
        )

    def part_start(kind, i):
        for d in range(1, n):
            part_copy(kind, i, d).start()

    def part_sum(kind, i):
        for d in range(1, n):
            part_copy(kind, i, d).wait()
        total = sends[rows_of(i, me), :].astype(F32)
        for d in range(1, n):
            total = total + parts[kind & 1, i, d - 1].astype(F32)
        return total

    def pass_copy(k, i, dst):
        return pltpu.make_async_remote_copy(
            src_ref=passed.at[i],
            dst_ref=dst,
            send_sem=pass_send.at[k, i],
            recv_sem=pass_recv.at[k, i],
            device_id={"section": 1 - section},
        )

    def row_mask(i):
        index = me * rows + lax.broadcasted_iota(jnp.int32, (rows, 1), 0)
        return index < lengths_ref[i]

    def enter(i):
        @pl.when(section == 1)
        def _():
            pass_copy(0, i, tokens.at[i]).wait_recv()

        unit, _ = normalize(tokens[i].astype(F32))
        normed[rows_of(i, me), :] = (unit * norms_ref[0:1, :] + norms_ref[1:2, :]).astype(BF)
        gather_start(0, normed, i)

    def attend(i):
        gather_wait(0, normed, i)
        here = image_of(i)
        for j in range(3):
            linear = mm(normed[here, :], w_qkv[j], 1, 1)
            if j == 0:
                linear = linear + time_ref[i, 0:1, :]
            if j == 2:
                linear = linear + time_ref[i, 1:2, :]
            qkv[j, here, :] = linear.astype(BF)
        key_index = lax.broadcasted_iota(jnp.int32, (1, seq), 1)
        key_mask = key_index < lengths_ref[i]
        outs = []
        for h in range(heads):
            lanes = slice(h * LANES, (h + 1) * LANES)
            scores = mm(qkv[0, here, lanes], qkv[1, here, lanes], 1, 1) * score_scale + bias[h]
            scores = jnp.where(key_mask, scores, NEG_FILL)
            top = jnp.max(scores, axis=-1, keepdims=True)
            raised = jnp.exp(scores - top)
            prob = raised / jnp.sum(raised, axis=-1, keepdims=True)
            probs[i * heads + h] = prob
            outs.append(mm(prob.astype(BF), qkv[2, here, lanes]).astype(BF))
        packed = mm(jnp.concatenate(outs, axis=1), selection(local, wide, head_size, True))
        packed = packed.astype(BF)
        mixed_heads[here, :] = packed
        sends[here, :] = mm(packed, w_out[...]).astype(BF)
        part_start(0, i)

    def middle(i):
        total = tokens[i].astype(F32) + part_sum(0, i) + out_b_ref[...]
        mixed[i] = total
        unit, _ = normalize(total)
        normed_two[rows_of(i, me), :] = (unit * norms_ref[2:3, :] + norms_ref[3:4, :]).astype(BF)
        gather_start(1, normed_two, i)

    def feed(i):
        gather_wait(1, normed_two, i)
        here = image_of(i)
        hidden = mm(normed_two[here, :], w_in[...]) + in_b_ref[...]
        square = hidden * hidden
        bent = jnp.tanh(ROOT * (hidden + CUBIC * (square * hidden)))
        half = 0.5 * (1.0 + bent)
        active[here, :] = (hidden * half).astype(BF)
        slope[here, :] = half + 0.5 * hidden * (1.0 - bent * bent) * (
            ROOT + (3.0 * CUBIC * ROOT) * square
        )
        sends[here, :] = mm(active[here, :], w_back[...]).astype(BF)
        part_start(1, i)

    def leave(i):
        out = mixed[i] + part_sum(1, i) + back_b_ref[...]

        @pl.when(section == 0)
        def _():
            passed[i] = out.astype(BF)
            pass_copy(0, i, tokens.at[i]).start()

        @pl.when(section == 1)
        def _():
            boundary_ref[0, i] = jnp.where(row_mask(i), out, 0.0)

    def grad_enter(i):
        @pl.when(section == 0)
        def _():
            pass_copy(1, i, grad_two.at[rows_of(i, me)]).wait_recv()
            gather_start(2, grad_two, i)

    def feed_back(i):
        @pl.when(section == 0)
        def _():
            gather_wait(2, grad_two, i)

        here = image_of(i)
        grad_active = mm(grad_two[here, :], w_back[...], 1, 1)
        held = (slope[here, :] * grad_active).astype(BF)
        grad_hidden[here, :] = held
        sums[6:7, :] += jnp.sum(held.astype(F32), axis=0, keepdims=True)
        sends[here, :] = mm(held, w_in[...], 1, 1).astype(BF)
        part_start(2, i)

    def middle_back(i):
        grad = part_sum(2, i)
        grad_y = grad_two[rows_of(i, me), :].astype(F32)
        grad_in, gain, offset = norm_backward(grad, mixed[i], norms_ref[2:3, :])
        total = grad_y + grad_in
        mixed[i] = total
        low = total.astype(BF)
        grad_one[rows_of(i, me), :] = low
        gather_start(3, grad_one, i)
        sums[2:3, :] += gain
        sums[3:4, :] += offset
        sums[4:5, :] += jnp.sum(low.astype(F32), axis=0, keepdims=True)
        sums[5:6, :] += jnp.sum(grad_y, axis=0, keepdims=True)

    def attend_back(i):
        gather_wait(3, grad_one, i)
        here = image_of(i)
        grad_heads = mm(grad_one[here, :], w_out[...], 1, 1).astype(BF)
        grad_heads = mm(grad_heads, selection(local, wide, head_size, False)).astype(BF)
        outs = ([], [], [])
        for h in range(heads):
            lanes = slice(h * LANES, (h + 1) * LANES)
            grad_out = grad_heads[:, lanes]
            prob = probs[i * heads + h]
            grad_prob = mm(grad_out, qkv[2, here, lanes], 1, 1)
            outs[2].append(mm(prob.astype(BF), grad_out, 0, 0).astype(BF))
            inner = jnp.sum(prob * grad_prob, axis=-1, keepdims=True)
            grad_scores = (prob * (grad_prob - inner)).astype(BF)
            score_sum[h, :, 0:seq] += grad_scores.astype(F32)
            outs[0].append((mm(grad_scores, qkv[1, here, lanes]) * score_scale).astype(BF))
            outs[1].append((mm(grad_scores, qkv[0, here, lanes], 0, 0) * score_scale).astype(BF))
        total = None
        chosen = selection(local, wide, head_size, True)
        for j in range(3):
            grad = jnp.concatenate(outs[j], axis=1)
            term = mm(grad, w_qkv[j])
            total = term if total is None else total + term
            grad_qkv[j, here, :] = mm(grad, chosen).astype(BF)
            if j != 1:
                columns_ref[replica, i, j // 2 : j // 2 + 1, :] = jnp.sum(
                    grad.astype(F32), axis=0, keepdims=True
                )
        sends[here, :] = total.astype(BF)
        part_start(3, i)

    def grad_leave(i):
        grad = part_sum(3, i)
        grad_in, gain, offset = norm_backward(grad, tokens[i].astype(F32), norms_ref[0:1, :])
        total = mixed[i] + grad_in

        @pl.when(section == 1)
        def _():
            passed[i] = total.astype(BF)
            pass_copy(1, i, grad_two.at[rows_of(i, me)]).start()

        @pl.when(section == 0)
        def _():
            boundary_ref[0, i] = total

        sums[0:1, :] += gain
        sums[1:2, :] += offset

    def each(body):
        def step(i, carry):
            body(i)
            return carry

        lax.fori_loop(0, count, step, 0)

    @pl.when(section == 0)
    def _():
        copy = pltpu.make_async_copy(images_ref, tokens, load_sem.at[4])
        copy.start()
        copy.wait()
        each(enter)

    @pl.when(section == 1)
    def _():
        copy = pltpu.make_async_copy(cotangent_ref, passed, load_sem.at[4])
        copy.start()
        copy.wait()

        def given(i):
            low = jnp.where(row_mask(i), passed[i].astype(F32), 0.0).astype(BF)
            grad_two[rows_of(i, me), :] = low
            gather_start(2, grad_two, i)

        each(given)

    sums[...] = jnp.zeros_like(sums)
    score_sum[...] = jnp.zeros_like(score_sum)
    for h in range(heads):
        spread = jnp.broadcast_to(table_ref[h : h + 1, :], (seq, 2 * seq))
        bias[h] = pltpu.roll(spread, seq + 1, 1, stride=1, stride_axis=0)[:, :seq]
    loads[0].wait()
    chosen = selection(local, wide, head_size, True)
    for j in range(3):
        w_qkv[j] = mm(chosen, w_raw[j * local : (j + 1) * local, :]).astype(BF)
    for load in loads[1:]:
        load.wait()

    @pl.when(section == 1)
    def _():
        each(lambda i: gather_wait(2, grad_two, i))

    def replica_peer(d):
        return lax.rem(replica + d, shares)

    def replica_source(d):
        return lax.rem(replica + shares - d, shares)

    def share_of(index):
        return pl.ds(pl.multiple_of(index * share, 8), share)

    jobs = (
        (w_raw, back_grad_ref),
        (w_back, in_grad_ref),
        (w_in, thin_grad_ref),
    )
    tile = width // 3
    paired = shares == 4
    half = replica // 2
    partner = replica + 1 - 2 * lax.rem(replica, 2)
    inner = (replica == 1) | (replica == 2)

    def across(c):
        return 2 - half if c else 3 * (1 - half)

    def own_copy(k):
        buf, dst = jobs[k]
        return pltpu.make_async_copy(
            buf.at[share_of(replica)], dst.at[0 if paired else replica], weight_own.at[k]
        )

    def weight_copy(k, index, dst, send, recv, device):
        return pltpu.make_async_remote_copy(
            src_ref=jobs[k][0].at[share_of(index)],
            dst_ref=dst,
            send_sem=weight_send.at[k, send],
            recv_sem=weight_recv.at[k, recv],
            device_id={"dp": device},
        )

    def near_copy(k):
        return weight_copy(k, partner, jobs[k][1].at[1], 0, 0, partner)

    def cross_copy(k, c):
        return weight_copy(k, across(c), crossed.at[k, c], 1 + c, 1 + c, partner)

    def forward_copy(k, c):
        return weight_copy(k, across(c), jobs[k][1].at[2], 1 + c, 3, across(c))

    def direct_copy(k, d, index):
        to = replica_peer(d)
        return weight_copy(k, to, jobs[k][1].at[index], d - 1, d - 1, to)

    def weight_step(k, t):
        place = 2 - t + half * (2 * t - 2) if paired else t
        where = pl.ds(pl.multiple_of(place * tile, LANES), tile)
        if k == 0:
            out = mm(grad_two[:, where], active[...], 0, 0)
        elif k == 1:
            out = mm(normed_two[:, where], grad_hidden[...], 0, 0)
        else:
            left = normed[:, where]
            out = [mm(left, grad_qkv[j], 0, 0) for j in range(3)]
            out.append(mm(grad_one[:, where], mixed_heads[...], 0, 0))
            out = jnp.concatenate(out, axis=1)
        jobs[k][0][where, :] = out.astype(BF)
        if paired:
            for c in range(2):

                @pl.when(jnp.logical_not(inner) & (t == c))
                def _(c=c):
                    cross_copy(k, c).start()

        @pl.when(t == 2)
        def _():
            own_copy(k).start()
            if paired:
                near_copy(k).start()
            else:
                for d in range(1, shares):
                    direct_copy(k, d, replica).start()

    def weight_job(k):
        def step(t, carry):
            weight_step(k, t)
            return carry

        lax.fori_loop(0, 3, step, 0)

    def relay(k):
        if paired:

            @pl.when(inner)
            def _():
                buf = jobs[k][0]
                for c in range(2):
                    where = share_of(across(c))
                    cross_copy(k, c).wait_recv()
                    pair = buf[where, :].astype(F32) + crossed[k, c].astype(F32)
                    buf[where, :] = pair.astype(BF)
                    forward_copy(k, c).start()

    def weight_wait(k):
        own_copy(k).wait()
        if paired:
            near_copy(k).wait()
            for c in range(2):
                cross_copy(k, c).wait_send()
            forward_copy(k, 0).wait_recv()
        else:
            for d in range(1, shares):
                direct_copy(k, d, replica).wait_send()
                direct_copy(k, d, replica_source(d)).wait_recv()

    def later_enter(i):
        @pl.when(section == 1)
        def _():
            enter(i)

    schedule = (
        (later_enter, 0, 0, count),
        (lambda i: weight_step(0, i), 14, 7, 3),
        (feed_back, 11, 8, count),
        (grad_enter, 8, 21, count),
        (lambda i: weight_step(1, i), 17, 10, 3),
        (attend, 1, 1, count),
        (grad_leave, 19, 19, count),
        (middle, 2, 2, count),
        (lambda i: relay(1), 22, 19, 1),
        (middle_back, 14, 14, count),
        (attend_back, 17, 16, count),
        (feed, 3, 4, count),
        (lambda i: weight_job(2), 19, 21, 1),
        (leave, 4, 7, count),
        (lambda i: relay(0), 18, 15, 1),
    )
    steps = max(max(first, second) for _, first, second, _ in schedule) + count

    def tick(t, carry):
        for body, first, second, times in schedule:
            i = t - (first + section * (second - first))

            @pl.when((i >= 0) & (i < times))
            def _(body=body, i=i):
                body(i)

        return carry

    lax.fori_loop(0, steps, tick, 0)

    @pl.when(section == 0)
    def _():
        each(lambda i: pass_copy(0, i, tokens.at[i]).wait_send())

    @pl.when(section == 1)
    def _():
        each(lambda i: pass_copy(1, i, grad_two.at[rows_of(i, me)]).wait_send())

    def sum_copy(d, index):
        return pltpu.make_async_remote_copy(
            src_ref=all_sums.at[me],
            dst_ref=all_sums.at[index],
            send_sem=sum_send.at[d - 1],
            recv_sem=sum_recv.at[d - 1],
            device_id={"mp": peer(d)},
        )

    all_sums[me] = sums[...]
    for d in range(1, n):
        sum_copy(d, me).start()

    lanes = 2 * seq
    carried = [jnp.zeros((8, lanes), F32) for _ in range(heads)]
    fill = jnp.zeros((8, lanes - score_sum.shape[2]), F32)

    def shift_add(g, carried):
        where = pl.ds(pl.multiple_of(g * 8, 8), 8)
        return [
            pltpu.roll(c, 8, 1) + jnp.concatenate([score_sum[h, where, :], fill], axis=1)
            for h, c in enumerate(carried)
        ]

    relay(2)
    carried = lax.fori_loop(0, seq // 8, shift_add, carried)
    behind = 7 - lax.broadcasted_iota(jnp.int32, (8, lanes), 0)
    for h in range(heads):
        c = carried[h]
        for by in (1, 2, 4):
            c = jnp.where((behind & by) != 0, pltpu.roll(c, by, 1), c)
        table_grad_ref[replica, h : h + 1, :] = jnp.sum(c, axis=0, keepdims=True)

    for d in range(1, n):
        sum_copy(d, me).wait_send()
        sum_copy(d, source(d)).wait_recv()
    total = all_sums[0]
    for k in range(1, n):
        total = total + all_sums[k]
    kind = lax.broadcasted_iota(jnp.int32, (8, width), 0)
    small_ref[replica] = jnp.where(kind < 6, total, sums[...])

    tiny = (small_ref, table_grad_ref, columns_ref, rows_ref)

    def tiny_copy(k, d, index):
        return pltpu.make_async_remote_copy(
            src_ref=tiny[k].at[replica],
            dst_ref=tiny[k].at[index],
            send_sem=tiny_send.at[k, d - 1],
            recv_sem=tiny_recv.at[k, d - 1],
            device_id={"dp": replica_peer(d)},
        )

    rows_ref[replica] = steps_ref[...]
    for k in range(4):
        for d in range(1, shares):
            tiny_copy(k, d, replica).start()
    for k in range(3):
        weight_wait(k)
    for k in range(4):
        for d in range(1, shares):
            tiny_copy(k, d, replica).wait_send()
            tiny_copy(k, d, replica_source(d)).wait_recv()


def run_layer(sizes, args):
    n, count, rows, width, hidden_width, heads, head_size, shares = sizes
    seq = n * rows
    local_width = heads * head_size
    wide = heads * LANES
    share = width // shares
    total = count * seq
    blocks = 3 if shares == 4 else shares
    vmem = pl.BlockSpec(memory_space=pltpu.VMEM)
    anywhere = pl.BlockSpec(memory_space=pl.ANY)
    dma = pltpu.SemaphoreType.DMA
    return pl.pallas_call(
        functools.partial(layer_kernel, sizes),
        out_shape=(
            jax.ShapeDtypeStruct((1, count, rows, width), F32),
            jax.ShapeDtypeStruct((shares, 8, width), F32),
            jax.ShapeDtypeStruct((shares, heads, 2 * seq), F32),
            jax.ShapeDtypeStruct((shares, count, 2, wide), F32),
            jax.ShapeDtypeStruct((shares, count, width), BF),
            jax.ShapeDtypeStruct((blocks, share, 4 * local_width), BF),
            jax.ShapeDtypeStruct((blocks, share, hidden_width), BF),
            jax.ShapeDtypeStruct((blocks, share, hidden_width), BF),
        ),
        in_specs=[
            pl.BlockSpec(memory_space=pltpu.SMEM),
            anywhere,
            anywhere,
            vmem,
            vmem,
            anywhere,
            anywhere,
            vmem,
            anywhere,
            vmem,
            anywhere,
            vmem,
            vmem,
            vmem,
        ],
        out_specs=(vmem, vmem, vmem, vmem, vmem, anywhere, anywhere, anywhere),
        scratch_shapes=[
            pltpu.VMEM((width, 4 * local_width), BF),
            pltpu.VMEM((3, wide, width), BF),
            pltpu.VMEM((local_width, width), BF),
            pltpu.VMEM((width, hidden_width), BF),
            pltpu.VMEM((hidden_width, width), BF),
            pltpu.VMEM((total, width), BF),
            pltpu.VMEM((total, width), BF),
            pltpu.VMEM((total, width), BF),
            pltpu.VMEM((total, width), BF),
            pltpu.VMEM((total, hidden_width), BF),
            pltpu.VMEM((total, hidden_width), BF),
            pltpu.VMEM((3, total, wide), BF),
            pltpu.VMEM((total, local_width), BF),
            pltpu.VMEM((3, total, local_width), BF),
            pltpu.VMEM((count * heads, seq, seq), F32),
            pltpu.VMEM((total, hidden_width), F32),
            pltpu.VMEM((heads, seq, seq), F32),
            pltpu.VMEM((heads, seq, -(-seq // LANES) * LANES), F32),
            pltpu.VMEM((2, count, n - 1, rows, width), BF),
            pltpu.VMEM((total, width), BF),
            pltpu.VMEM((count, rows, width), BF),
            pltpu.VMEM((count, rows, width), BF),
            pltpu.VMEM((count, rows, width), F32),
            pltpu.VMEM((3, 2, share, hidden_width), BF),
            pltpu.VMEM((8, width), F32),
            pltpu.VMEM((n, 8, width), F32),
            dma((5,)),
            dma((4, count, n - 1)),
            dma((4, count, n - 1)),
            dma((4, count, n - 1)),
            dma((4, count, n - 1)),
            dma((2, count)),
            dma((2, count)),
            dma((3, shares)),
            dma((3, shares)),
            dma((3,)),
            dma((4, shares - 1)),
            dma((4, shares - 1)),
            dma((n - 1,)),
            dma((n - 1,)),
        ],
        compiler_params=pltpu.CompilerParams(
            collective_id=0, has_side_effects=True, vmem_limit_bytes=67043328
        ),
        name="two_pass",
    )(*args)


def local(
    images,
    cotangent,
    lengths,
    timesteps,
    time_table,
    norms,
    qkv_weight,
    time_weight,
    out_weight,
    out_bias,
    mlp_in_weight,
    mlp_in_bias,
    mlp_out_weight,
    mlp_out_bias,
    rel_bias,
):
    count, rows, width = images.shape
    local_width = qkv_weight.shape[3]
    hidden_width = mlp_in_weight.shape[2]
    heads = rel_bias.shape[1]
    head_size = local_width // heads
    shares = lax.axis_size("dp")
    share = width // shares
    sizes = (lax.axis_size("mp"), count, rows, width, hidden_width, heads, head_size, shares)
    chosen = jax.nn.one_hot(timesteps, time_table.shape[0], dtype=BF)
    time_rows = jnp.dot(chosen, time_table, preferred_element_type=F32).astype(BF)
    time_part = jnp.dot(
        time_rows, time_weight[0].reshape(width, 2 * local_width), preferred_element_type=F32
    ).reshape(count, 2, heads, head_size)
    time_part = jnp.pad(time_part, ((0, 0), (0, 0), (0, 0), (0, LANES - head_size)))
    time_part = time_part.reshape(count, 2, heads * LANES)
    table = jnp.pad(jnp.flip(rel_bias[0], axis=1), ((0, 0), (0, 1)))
    outs = run_layer(
        sizes,
        (
            lengths,
            images,
            cotangent,
            time_part,
            norms[0],
            jnp.transpose(qkv_weight[0], (1, 2, 0)).reshape(3 * local_width, width),
            out_weight[0],
            out_bias,
            mlp_in_weight[0],
            mlp_in_bias,
            mlp_out_weight[0],
            mlp_out_bias,
            table,
            time_rows,
        ),
    )
    boundary, small, table_grad, columns, all_rows, thin_grad, in_grad, back_grad = outs
    columns = columns.reshape(shares * count, 2, heads, LANES)[..., :head_size]
    columns = columns.reshape(shares * count, 2 * local_width)
    all_rows = lax.dynamic_slice_in_dim(
        all_rows.reshape(shares * count, width), lax.axis_index("dp") * share, share, axis=1
    )
    time_grad = lax.dot_general(
        all_rows.astype(F32),
        columns,
        (((0,), (0,)), ((), ())),
        precision=lax.Precision.HIGHEST,
        preferred_element_type=F32,
    ).reshape(share, 2, local_width)

    def added(value):
        return functools.reduce(jnp.add, [value[k].astype(F32) for k in range(value.shape[0])])

    small = added(small)
    thin_parts = [
        added(thin_grad[:, :, j * local_width : (j + 1) * local_width]) for j in range(4)
    ]
    table_grad = jnp.flip(added(table_grad)[:, : rel_bias.shape[2]], axis=1)
    return (
        boundary,
        small[None, :4],
        jnp.transpose(jnp.stack(thin_parts[:3]), (1, 0, 2))[None],
        time_grad[None],
        thin_parts[3].T[None],
        small[4][None],
        added(in_grad)[None],
        small[6][None],
        added(back_grad).T[None],
        small[5][None],
        table_grad[None],
    )


def solution(mesh):
    in_specs = (
        P("dp", "mp", None),
        P("dp", "mp", None),
        P("dp"),
        P("dp"),
        P(),
        P("section", None, None),
        P("section", None, None, "mp"),
        P("section", None, None, "mp"),
        P("section", "mp", None),
        P("section", None),
        P("section", None, "mp"),
        P("section", "mp"),
        P("section", "mp", None),
        P("section", None),
        P("section", "mp", None),
    )
    out_specs = (
        P("section", "dp", "mp", None),
        P("section", None, None),
        P("section", "dp", None, "mp"),
        P("section", "dp", None, "mp"),
        P("section", "mp", "dp"),
        P("section", None),
        P("section", "dp", "mp"),
        P("section", "mp"),
        P("section", "mp", "dp"),
        P("section", None),
        P("section", "mp", None),
    )
    return jax.shard_map(local, mesh=mesh, in_specs=in_specs, out_specs=out_specs, check_vma=False)
```

```python
import functools
import math

import jax
import jax.numpy as jnp
from jax import lax
from jax.experimental import pallas as pl
from jax.experimental.pallas import tpu as pltpu
from jax.sharding import PartitionSpec as P

EPSILON = 1e-06
NEG_FILL = -1000000000.0
LANES = 128
BF = jnp.bfloat16
F32 = jnp.float32
ROOT = math.sqrt(2.0 / math.pi)
CUBIC = 0.044715


def mm(left, right, left_dim=1, right_dim=0):
    return lax.dot_general(
        left, right, (((left_dim,), (right_dim,)), ((), ())), preferred_element_type=F32
    )


def selection(rows, cols, head_size, flip):
    shape = (cols, rows) if flip else (rows, cols)
    row = lax.broadcasted_iota(jnp.int32, shape, 1 if flip else 0)
    col = lax.broadcasted_iota(jnp.int32, shape, 0 if flip else 1)
    within = col & (LANES - 1)
    hit = (within < head_size) & (row == (col // LANES) * head_size + within)
    return jnp.where(hit, 1.0, 0.0).astype(BF)


def normalize(values):
    centred = values - jnp.mean(values, axis=-1, keepdims=True)
    spread = jnp.mean(centred * centred, axis=-1, keepdims=True)
    scale = lax.rsqrt(spread + EPSILON)
    return centred * scale, scale


def norm_backward(grad, values, gain):
    unit, scale = normalize(values)
    inner = grad * gain
    mean_one = jnp.mean(inner, axis=-1, keepdims=True)
    mean_two = jnp.mean(inner * unit, axis=-1, keepdims=True)
    grad_in = scale * (inner - mean_one - unit * mean_two)
    gain_grad = jnp.sum(grad * unit, axis=0, keepdims=True)
    offset_grad = jnp.sum(grad, axis=0, keepdims=True)
    return grad_in, gain_grad, offset_grad


def layer_kernel(
    sizes,
    lengths_ref,
    images_ref,
    cotangent_ref,
    time_ref,
    norms_ref,
    qkv_raw_ref,
    out_w_ref,
    out_b_ref,
    in_w_ref,
    in_b_ref,
    back_w_ref,
    back_b_ref,
    table_ref,
    steps_ref,
    boundary_ref,
    small_ref,
    table_grad_ref,
    columns_ref,
    rows_ref,
    thin_grad_ref,
    in_grad_ref,
    back_grad_ref,
    w_raw,
    w_qkv,
    w_out,
    w_in,
    w_back,
    normed,
    normed_two,
    grad_two,
    grad_one,
    active,
    grad_hidden,
    qkv,
    mixed_heads,
    grad_qkv,
    probs,
    slope,
    bias,
    score_sum,
    parts,
    sends,
    tokens,
    passed,
    mixed,
    crossed,
    sums,
    all_sums,
    load_sem,
    gather_send,
    gather_recv,
    part_send,
    part_recv,
    pass_send,
    pass_recv,
    weight_send,
    weight_recv,
    weight_own,
    tiny_send,
    tiny_recv,
    sum_send,
    sum_recv,
):
    n, count, rows, width, hidden_width, heads, head_size, shares = sizes
    seq = n * rows
    local = heads * head_size
    wide = heads * LANES
    share = width // shares
    score_scale = 1.0 / math.sqrt(head_size)
    me = lax.axis_index("mp")
    section = lax.axis_index("section")
    replica = lax.axis_index("dp")
    own = pl.multiple_of(me * rows, 16)

    def peer(d):
        if n == 4:
            return (n - 1 - me, me + 1 - 2 * lax.rem(me, 2), lax.rem(me + 2, n))[d - 1]
        return lax.rem(me + d, n)

    def source(d):
        return peer(d) if n == 4 else lax.rem(me + n - d, n)

    barrier = pltpu.get_barrier_semaphore()
    for d in range(1, n):
        pl.semaphore_signal(barrier, inc=1, device_id={"mp": peer(d)})
    pl.semaphore_signal(barrier, inc=1, device_id={"section": 1 - section})
    for d in range(1, shares):
        pl.semaphore_signal(barrier, inc=1, device_id={"dp": lax.rem(replica + d, shares)})
    pl.semaphore_wait(barrier, n + shares - 1)

    loads = [
        pltpu.make_async_copy(a, b, load_sem.at[k])
        for k, (a, b) in enumerate(
            [(qkv_raw_ref, w_raw.at[0 : 3 * local]), (out_w_ref, w_out), (in_w_ref, w_in), (back_w_ref, w_back)]
        )
    ]
    for load in loads:
        load.start()

    def rows_of(i, index):
        return pl.ds(pl.multiple_of(i * seq + index * rows, 16), rows)

    def image_of(i):
        return pl.ds(pl.multiple_of(i * seq, 16), seq)

    def gather_copy(kind, buf, i, d, index):
        where = rows_of(i, index)
        return pltpu.make_async_remote_copy(
            src_ref=buf.at[where],
            dst_ref=buf.at[where],
            send_sem=gather_send.at[kind, i, d - 1],
            recv_sem=gather_recv.at[kind, i, d - 1],
            device_id={"mp": peer(d)},
        )

    def gather_start(kind, buf, i):
        for d in range(1, n):
            gather_copy(kind, buf, i, d, me).start()

    def gather_wait(kind, buf, i):
        for d in range(1, n):
            gather_copy(kind, buf, i, d, me).wait_send()
            gather_copy(kind, buf, i, d, source(d)).wait_recv()

    def part_copy(kind, i, d):
        return pltpu.make_async_remote_copy(
            src_ref=sends.at[rows_of(i, peer(d))],
            dst_ref=parts.at[kind & 1, i, d - 1],
            send_sem=part_send.at[kind, i, d - 1],
            recv_sem=part_recv.at[kind, i, d - 1],
            device_id={"mp": peer(d)},
        )

    def part_start(kind, i):
        for d in range(1, n):
            part_copy(kind, i, d).start()

    def part_sum(kind, i):
        for d in range(1, n):
            part_copy(kind, i, d).wait()
        total = sends[rows_of(i, me), :].astype(F32)
        for d in range(1, n):
            total = total + parts[kind & 1, i, d - 1].astype(F32)
        return total

    def pass_copy(k, i, dst):
        return pltpu.make_async_remote_copy(
            src_ref=passed.at[i],
            dst_ref=dst,
            send_sem=pass_send.at[k, i],
            recv_sem=pass_recv.at[k, i],
            device_id={"section": 1 - section},
        )

    def row_mask(i):
        index = me * rows + lax.broadcasted_iota(jnp.int32, (rows, 1), 0)
        return index < lengths_ref[i]

    def enter(i):
        @pl.when(section == 1)
        def _():
            pass_copy(0, i, tokens.at[i]).wait_recv()

        unit, _ = normalize(tokens[i].astype(F32))
        normed[rows_of(i, me), :] = (unit * norms_ref[0:1, :] + norms_ref[1:2, :]).astype(BF)
        gather_start(0, normed, i)

    def attend(i):
        gather_wait(0, normed, i)
        here = image_of(i)
        for j in range(3):
            linear = mm(normed[here, :], w_qkv[j], 1, 1)
            if j == 0:
                linear = linear + time_ref[i, 0:1, :]
            if j == 2:
                linear = linear + time_ref[i, 1:2, :]
            qkv[j, here, :] = linear.astype(BF)
        key_index = lax.broadcasted_iota(jnp.int32, (1, seq), 1)
        key_mask = key_index < lengths_ref[i]
        outs = []
        for h in range(heads):
            lanes = slice(h * LANES, (h + 1) * LANES)
            scores = mm(qkv[0, here, lanes], qkv[1, here, lanes], 1, 1) * score_scale + bias[h]
            scores = jnp.where(key_mask, scores, NEG_FILL)
            top = jnp.max(scores, axis=-1, keepdims=True)
            raised = jnp.exp(scores - top)
            prob = raised / jnp.sum(raised, axis=-1, keepdims=True)
            probs[i * heads + h] = prob
            outs.append(mm(prob.astype(BF), qkv[2, here, lanes]).astype(BF))
        packed = mm(jnp.concatenate(outs, axis=1), selection(local, wide, head_size, True))
        packed = packed.astype(BF)
        mixed_heads[here, :] = packed
        sends[here, :] = mm(packed, w_out[...]).astype(BF)
        part_start(0, i)

    def middle(i):
        total = tokens[i].astype(F32) + part_sum(0, i) + out_b_ref[...]
        mixed[i] = total
        unit, _ = normalize(total)
        normed_two[rows_of(i, me), :] = (unit * norms_ref[2:3, :] + norms_ref[3:4, :]).astype(BF)
        gather_start(1, normed_two, i)

    def feed(i):
        gather_wait(1, normed_two, i)
        here = image_of(i)
        hidden = mm(normed_two[here, :], w_in[...]) + in_b_ref[...]
        square = hidden * hidden
        bent = jnp.tanh(ROOT * (hidden + CUBIC * (square * hidden)))
        half = 0.5 * (1.0 + bent)
        active[here, :] = (hidden * half).astype(BF)
        slope[here, :] = half + 0.5 * hidden * (1.0 - bent * bent) * (
            ROOT + (3.0 * CUBIC * ROOT) * square
        )
        sends[here, :] = mm(active[here, :], w_back[...]).astype(BF)
        part_start(1, i)

    def leave(i):
        out = mixed[i] + part_sum(1, i) + back_b_ref[...]

        @pl.when(section == 0)
        def _():
            passed[i] = out.astype(BF)
            pass_copy(0, i, tokens.at[i]).start()

        @pl.when(section == 1)
        def _():
            boundary_ref[0, i] = jnp.where(row_mask(i), out, 0.0)

    def grad_enter(i):
        @pl.when(section == 0)
        def _():
            pass_copy(1, i, grad_two.at[rows_of(i, me)]).wait_recv()
            gather_start(2, grad_two, i)

    def feed_back(i):
        @pl.when(section == 0)
        def _():
            gather_wait(2, grad_two, i)

        here = image_of(i)
        grad_active = mm(grad_two[here, :], w_back[...], 1, 1)
        held = (slope[here, :] * grad_active).astype(BF)
        grad_hidden[here, :] = held
        sums[6:7, :] += jnp.sum(held.astype(F32), axis=0, keepdims=True)
        sends[here, :] = mm(held, w_in[...], 1, 1).astype(BF)
        part_start(2, i)

    def middle_back(i):
        grad = part_sum(2, i)
        grad_y = grad_two[rows_of(i, me), :].astype(F32)
        grad_in, gain, offset = norm_backward(grad, mixed[i], norms_ref[2:3, :])
        total = grad_y + grad_in
        mixed[i] = total
        low = total.astype(BF)
        grad_one[rows_of(i, me), :] = low
        gather_start(3, grad_one, i)
        sums[2:3, :] += gain
        sums[3:4, :] += offset
        sums[4:5, :] += jnp.sum(low.astype(F32), axis=0, keepdims=True)
        sums[5:6, :] += jnp.sum(grad_y, axis=0, keepdims=True)

    def attend_back(i):
        gather_wait(3, grad_one, i)
        here = image_of(i)
        grad_heads = mm(grad_one[here, :], w_out[...], 1, 1).astype(BF)
        grad_heads = mm(grad_heads, selection(local, wide, head_size, False)).astype(BF)
        outs = ([], [], [])
        for h in range(heads):
            lanes = slice(h * LANES, (h + 1) * LANES)
            grad_out = grad_heads[:, lanes]
            prob = probs[i * heads + h]
            grad_prob = mm(grad_out, qkv[2, here, lanes], 1, 1)
            outs[2].append(mm(prob.astype(BF), grad_out, 0, 0).astype(BF))
            inner = jnp.sum(prob * grad_prob, axis=-1, keepdims=True)
            grad_scores = (prob * (grad_prob - inner)).astype(BF)
            score_sum[h, :, 0:seq] += grad_scores.astype(F32)
            outs[0].append((mm(grad_scores, qkv[1, here, lanes]) * score_scale).astype(BF))
            outs[1].append((mm(grad_scores, qkv[0, here, lanes], 0, 0) * score_scale).astype(BF))
        total = None
        chosen = selection(local, wide, head_size, True)
        for j in range(3):
            grad = jnp.concatenate(outs[j], axis=1)
            term = mm(grad, w_qkv[j])
            total = term if total is None else total + term
            grad_qkv[j, here, :] = mm(grad, chosen).astype(BF)
            if j != 1:
                columns_ref[replica, i, j // 2 : j // 2 + 1, :] = jnp.sum(
                    grad.astype(F32), axis=0, keepdims=True
                )
        sends[here, :] = total.astype(BF)
        part_start(3, i)

    def grad_leave(i):
        grad = part_sum(3, i)
        grad_in, gain, offset = norm_backward(grad, tokens[i].astype(F32), norms_ref[0:1, :])
        total = mixed[i] + grad_in

        @pl.when(section == 1)
        def _():
            passed[i] = total.astype(BF)
            pass_copy(1, i, grad_two.at[rows_of(i, me)]).start()

        @pl.when(section == 0)
        def _():
            boundary_ref[0, i] = total

        sums[0:1, :] += gain
        sums[1:2, :] += offset

    def each(body):
        def step(i, carry):
            body(i)
            return carry

        lax.fori_loop(0, count, step, 0)

    @pl.when(section == 0)
    def _():
        copy = pltpu.make_async_copy(images_ref, tokens, load_sem.at[4])
        copy.start()
        copy.wait()
        each(enter)

    @pl.when(section == 1)
    def _():
        copy = pltpu.make_async_copy(cotangent_ref, passed, load_sem.at[4])
        copy.start()
        copy.wait()

        def given(i):
            low = jnp.where(row_mask(i), passed[i].astype(F32), 0.0).astype(BF)
            grad_two[rows_of(i, me), :] = low
            gather_start(2, grad_two, i)

        each(given)

    sums[...] = jnp.zeros_like(sums)
    score_sum[...] = jnp.zeros_like(score_sum)
    for h in range(heads):
        spread = jnp.broadcast_to(table_ref[h : h + 1, :], (seq, 2 * seq))
        bias[h] = pltpu.roll(spread, seq + 1, 1, stride=1, stride_axis=0)[:, :seq]
    loads[0].wait()
    chosen = selection(local, wide, head_size, True)
    for j in range(3):
        w_qkv[j] = mm(chosen, w_raw[j * local : (j + 1) * local, :]).astype(BF)
    for load in loads[1:]:
        load.wait()

    @pl.when(section == 1)
    def _():
        each(lambda i: gather_wait(2, grad_two, i))

    def replica_peer(d):
        return lax.rem(replica + d, shares)

    def replica_source(d):
        return lax.rem(replica + shares - d, shares)

    def share_of(index):
        return pl.ds(pl.multiple_of(index * share, 8), share)

    jobs = (
        (w_raw, back_grad_ref),
        (w_back, in_grad_ref),
        (w_in, thin_grad_ref),
    )
    tile = width // 3
    paired = shares == 4
    half = replica // 2
    partner = replica + 1 - 2 * lax.rem(replica, 2)
    inner = (replica == 1) | (replica == 2)

    def across(c):
        return 2 - half if c else 3 * (1 - half)

    def own_copy(k):
        buf, dst = jobs[k]
        return pltpu.make_async_copy(
            buf.at[share_of(replica)], dst.at[0 if paired else replica], weight_own.at[k]
        )

    def weight_copy(k, index, dst, send, recv, device):
        return pltpu.make_async_remote_copy(
            src_ref=jobs[k][0].at[share_of(index)],
            dst_ref=dst,
            send_sem=weight_send.at[k, send],
            recv_sem=weight_recv.at[k, recv],
            device_id={"dp": device},
        )

    def near_copy(k):
        return weight_copy(k, partner, jobs[k][1].at[1], 0, 0, partner)

    def cross_copy(k, c):
        return weight_copy(k, across(c), crossed.at[k, c], 1 + c, 1 + c, partner)

    def forward_copy(k, c):
        return weight_copy(k, across(c), jobs[k][1].at[2], 1 + c, 3, across(c))

    def direct_copy(k, d, index):
        to = replica_peer(d)
        return weight_copy(k, to, jobs[k][1].at[index], d - 1, d - 1, to)

    def weight_step(k, t):
        place = 2 - t + half * (2 * t - 2) if paired else t
        where = pl.ds(pl.multiple_of(place * tile, LANES), tile)
        if k == 0:
            out = mm(grad_two[:, where], active[...], 0, 0)
        elif k == 1:
            out = mm(normed_two[:, where], grad_hidden[...], 0, 0)
        else:
            left = normed[:, where]
            out = [mm(left, grad_qkv[j], 0, 0) for j in range(3)]
            out.append(mm(grad_one[:, where], mixed_heads[...], 0, 0))
            out = jnp.concatenate(out, axis=1)
        jobs[k][0][where, :] = out.astype(BF)
        if paired:
            for c in range(2):

                @pl.when(jnp.logical_not(inner) & (t == c))
                def _(c=c):
                    cross_copy(k, c).start()

        @pl.when(t == 2)
        def _():
            own_copy(k).start()
            if paired:
                near_copy(k).start()
            else:
                for d in range(1, shares):
                    direct_copy(k, d, replica).start()

    def relay(k):
        if paired:

            @pl.when(inner)
            def _():
                buf = jobs[k][0]
                for c in range(2):
                    where = share_of(across(c))
                    cross_copy(k, c).wait_recv()
                    pair = buf[where, :].astype(F32) + crossed[k, c].astype(F32)
                    buf[where, :] = pair.astype(BF)
                    forward_copy(k, c).start()

    def weight_wait(k):
        own_copy(k).wait()
        if paired:
            near_copy(k).wait()
            for c in range(2):
                cross_copy(k, c).wait_send()
            forward_copy(k, 0).wait_recv()
        else:
            for d in range(1, shares):
                direct_copy(k, d, replica).wait_send()
                direct_copy(k, d, replica_source(d)).wait_recv()

    def later_enter(i):
        @pl.when(section == 1)
        def _():
            enter(i)

    schedule = (
        (later_enter, 0, 0, count),
        (lambda i: weight_step(0, i), 14, 7, 3),
        (feed_back, 11, 8, count),
        (grad_enter, 8, 21, count),
        (lambda i: weight_step(1, i), 17, 10, 3),
        (attend, 1, 1, count),
        (grad_leave, 19, 19, count),
        (middle, 2, 2, count),
        (lambda i: relay(1), 22, 19, 1),
        (middle_back, 14, 14, count),
        (attend_back, 17, 16, count),
        (feed, 3, 4, count),
        (lambda i: weight_step(2, i), 19, 19, 3),
        (leave, 4, 7, count),
        (lambda i: relay(0), 18, 15, 1),
    )
    steps = max(max(first, second) for _, first, second, _ in schedule) + count

    def tick(t, carry):
        for body, first, second, times in schedule:
            i = t - (first + section * (second - first))

            @pl.when((i >= 0) & (i < times))
            def _(body=body, i=i):
                body(i)

        return carry

    lax.fori_loop(0, steps, tick, 0)

    @pl.when(section == 0)
    def _():
        each(lambda i: pass_copy(0, i, tokens.at[i]).wait_send())

    @pl.when(section == 1)
    def _():
        each(lambda i: pass_copy(1, i, grad_two.at[rows_of(i, me)]).wait_send())

    def sum_copy(d, index):
        return pltpu.make_async_remote_copy(
            src_ref=all_sums.at[me],
            dst_ref=all_sums.at[index],
            send_sem=sum_send.at[d - 1],
            recv_sem=sum_recv.at[d - 1],
            device_id={"mp": peer(d)},
        )

    all_sums[me] = sums[...]
    for d in range(1, n):
        sum_copy(d, me).start()

    lanes = 2 * seq
    carried = [jnp.zeros((8, lanes), F32) for _ in range(heads)]
    fill = jnp.zeros((8, lanes - score_sum.shape[2]), F32)

    def shift_add(g, carried):
        where = pl.ds(pl.multiple_of(g * 8, 8), 8)
        return [
            pltpu.roll(c, 8, 1) + jnp.concatenate([score_sum[h, where, :], fill], axis=1)
            for h, c in enumerate(carried)
        ]

    relay(2)
    carried = lax.fori_loop(0, seq // 8, shift_add, carried)
    behind = 7 - lax.broadcasted_iota(jnp.int32, (8, lanes), 0)
    for h in range(heads):
        c = carried[h]
        for by in (1, 2, 4):
            c = jnp.where((behind & by) != 0, pltpu.roll(c, by, 1), c)
        table_grad_ref[replica, h : h + 1, :] = jnp.sum(c, axis=0, keepdims=True)

    for d in range(1, n):
        sum_copy(d, me).wait_send()
        sum_copy(d, source(d)).wait_recv()
    total = all_sums[0]
    for k in range(1, n):
        total = total + all_sums[k]
    kind = lax.broadcasted_iota(jnp.int32, (8, width), 0)
    small_ref[replica] = jnp.where(kind < 6, total, sums[...])

    tiny = (small_ref, table_grad_ref, columns_ref, rows_ref)

    def tiny_copy(k, d, index):
        return pltpu.make_async_remote_copy(
            src_ref=tiny[k].at[replica],
            dst_ref=tiny[k].at[index],
            send_sem=tiny_send.at[k, d - 1],
            recv_sem=tiny_recv.at[k, d - 1],
            device_id={"dp": replica_peer(d)},
        )

    rows_ref[replica] = steps_ref[...]
    for k in range(4):
        for d in range(1, shares):
            tiny_copy(k, d, replica).start()
    for k in range(3):
        weight_wait(k)
    for k in range(4):
        for d in range(1, shares):
            tiny_copy(k, d, replica).wait_send()
            tiny_copy(k, d, replica_source(d)).wait_recv()


def run_layer(sizes, args):
    n, count, rows, width, hidden_width, heads, head_size, shares = sizes
    seq = n * rows
    local_width = heads * head_size
    wide = heads * LANES
    share = width // shares
    total = count * seq
    blocks = 3 if shares == 4 else shares
    vmem = pl.BlockSpec(memory_space=pltpu.VMEM)
    anywhere = pl.BlockSpec(memory_space=pl.ANY)
    dma = pltpu.SemaphoreType.DMA
    return pl.pallas_call(
        functools.partial(layer_kernel, sizes),
        out_shape=(
            jax.ShapeDtypeStruct((1, count, rows, width), F32),
            jax.ShapeDtypeStruct((shares, 8, width), F32),
            jax.ShapeDtypeStruct((shares, heads, 2 * seq), F32),
            jax.ShapeDtypeStruct((shares, count, 2, wide), F32),
            jax.ShapeDtypeStruct((shares, count, width), BF),
            jax.ShapeDtypeStruct((blocks, share, 4 * local_width), BF),
            jax.ShapeDtypeStruct((blocks, share, hidden_width), BF),
            jax.ShapeDtypeStruct((blocks, share, hidden_width), BF),
        ),
        in_specs=[
            pl.BlockSpec(memory_space=pltpu.SMEM),
            anywhere,
            anywhere,
            vmem,
            vmem,
            anywhere,
            anywhere,
            vmem,
            anywhere,
            vmem,
            anywhere,
            vmem,
            vmem,
            vmem,
        ],
        out_specs=(vmem, vmem, vmem, vmem, vmem, anywhere, anywhere, anywhere),
        scratch_shapes=[
            pltpu.VMEM((width, 4 * local_width), BF),
            pltpu.VMEM((3, wide, width), BF),
            pltpu.VMEM((local_width, width), BF),
            pltpu.VMEM((width, hidden_width), BF),
            pltpu.VMEM((hidden_width, width), BF),
            pltpu.VMEM((total, width), BF),
            pltpu.VMEM((total, width), BF),
            pltpu.VMEM((total, width), BF),
            pltpu.VMEM((total, width), BF),
            pltpu.VMEM((total, hidden_width), BF),
            pltpu.VMEM((total, hidden_width), BF),
            pltpu.VMEM((3, total, wide), BF),
            pltpu.VMEM((total, local_width), BF),
            pltpu.VMEM((3, total, local_width), BF),
            pltpu.VMEM((count * heads, seq, seq), F32),
            pltpu.VMEM((total, hidden_width), F32),
            pltpu.VMEM((heads, seq, seq), F32),
            pltpu.VMEM((heads, seq, -(-seq // LANES) * LANES), F32),
            pltpu.VMEM((2, count, n - 1, rows, width), BF),
            pltpu.VMEM((total, width), BF),
            pltpu.VMEM((count, rows, width), BF),
            pltpu.VMEM((count, rows, width), BF),
            pltpu.VMEM((count, rows, width), F32),
            pltpu.VMEM((3, 2, share, hidden_width), BF),
            pltpu.VMEM((8, width), F32),
            pltpu.VMEM((n, 8, width), F32),
            dma((5,)),
            dma((4, count, n - 1)),
            dma((4, count, n - 1)),
            dma((4, count, n - 1)),
            dma((4, count, n - 1)),
            dma((2, count)),
            dma((2, count)),
            dma((3, shares)),
            dma((3, shares)),
            dma((3,)),
            dma((4, shares - 1)),
            dma((4, shares - 1)),
            dma((n - 1,)),
            dma((n - 1,)),
        ],
        compiler_params=pltpu.CompilerParams(
            collective_id=0, has_side_effects=True, vmem_limit_bytes=67043328
        ),
        name="two_pass",
    )(*args)


def local(
    images,
    cotangent,
    lengths,
    timesteps,
    time_table,
    norms,
    qkv_weight,
    time_weight,
    out_weight,
    out_bias,
    mlp_in_weight,
    mlp_in_bias,
    mlp_out_weight,
    mlp_out_bias,
    rel_bias,
):
    count, rows, width = images.shape
    local_width = qkv_weight.shape[3]
    hidden_width = mlp_in_weight.shape[2]
    heads = rel_bias.shape[1]
    head_size = local_width // heads
    shares = lax.axis_size("dp")
    share = width // shares
    sizes = (lax.axis_size("mp"), count, rows, width, hidden_width, heads, head_size, shares)
    chosen = jax.nn.one_hot(timesteps, time_table.shape[0], dtype=BF)
    time_rows = jnp.dot(chosen, time_table, preferred_element_type=F32).astype(BF)
    time_part = jnp.dot(
        time_rows, time_weight[0].reshape(width, 2 * local_width), preferred_element_type=F32
    ).reshape(count, 2, heads, head_size)
    time_part = jnp.pad(time_part, ((0, 0), (0, 0), (0, 0), (0, LANES - head_size)))
    time_part = time_part.reshape(count, 2, heads * LANES)
    table = jnp.pad(jnp.flip(rel_bias[0], axis=1), ((0, 0), (0, 1)))
    outs = run_layer(
        sizes,
        (
            lengths,
            images,
            cotangent,
            time_part,
            norms[0],
            jnp.transpose(qkv_weight[0], (1, 2, 0)).reshape(3 * local_width, width),
            out_weight[0],
            out_bias,
            mlp_in_weight[0],
            mlp_in_bias,
            mlp_out_weight[0],
            mlp_out_bias,
            table,
            time_rows,
        ),
    )
    boundary, small, table_grad, columns, all_rows, thin_grad, in_grad, back_grad = outs
    columns = columns.reshape(shares * count, 2, heads, LANES)[..., :head_size]
    columns = columns.reshape(shares * count, 2 * local_width)
    all_rows = lax.dynamic_slice_in_dim(
        all_rows.reshape(shares * count, width), lax.axis_index("dp") * share, share, axis=1
    )
    time_grad = lax.dot_general(
        all_rows.astype(F32),
        columns,
        (((0,), (0,)), ((), ())),
        precision=lax.Precision.HIGHEST,
        preferred_element_type=F32,
    ).reshape(share, 2, local_width)

    def added(value):
        return functools.reduce(jnp.add, [value[k].astype(F32) for k in range(value.shape[0])])

    small = added(small)
    thin_parts = [
        added(thin_grad[:, :, j * local_width : (j + 1) * local_width]) for j in range(4)
    ]
    table_grad = jnp.flip(added(table_grad)[:, : rel_bias.shape[2]], axis=1)
    return (
        boundary,
        small[None, :4],
        jnp.transpose(jnp.stack(thin_parts[:3]), (1, 0, 2))[None],
        time_grad[None],
        thin_parts[3].T[None],
        small[4][None],
        added(in_grad)[None],
        small[6][None],
        added(back_grad).T[None],
        small[5][None],
        table_grad[None],
    )


def solution(mesh):
    in_specs = (
        P("dp", "mp", None),
        P("dp", "mp", None),
        P("dp"),
        P("dp"),
        P(),
        P("section", None, None),
        P("section", None, None, "mp"),
        P("section", None, None, "mp"),
        P("section", "mp", None),
        P("section", None),
        P("section", None, "mp"),
        P("section", "mp"),
        P("section", "mp", None),
        P("section", None),
        P("section", "mp", None),
    )
    out_specs = (
        P("section", "dp", "mp", None),
        P("section", None, None),
        P("section", "dp", None, "mp"),
        P("section", "dp", None, "mp"),
        P("section", "mp", "dp"),
        P("section", None),
        P("section", "dp", "mp"),
        P("section", "mp"),
        P("section", "mp", "dp"),
        P("section", None),
        P("section", "mp", None),
    )
    return jax.shard_map(local, mesh=mesh, in_specs=in_specs, out_specs=out_specs, check_vma=False)
```
